32 devices in a mesh: dp: 1 (over z), tp: 32 (over y, x, core).
Axes of the slice: x: 4, y: 4, z: 1, core: 2. Of those that a mesh axis runs over, the one named last changes fastest.
The devices are a block of a 4x4x8 slice.
Arguments:
- token_ids: int32 [16384], P('dp')
- embed_table: bfloat16 [50304, 768], P('tp')
- norm_gain: bfloat16 [768], replicated
- w_in: bfloat16 [768, 3072], P(None, 'tp')
- w_out: bfloat16 [3072, 768], P('tp')
Outputs:
- output: bfloat16 [16384, 768], P(('dp', 'tp'))
All inputs are finite; a program needn't handle non-finite values.
Results may differ from the reference program's by a relative error of at most 0.00790572.
Values are sent between devices in bfloat16 or wider.
A program may use at most 768 MiB of HBM per device.

```python
import math
import jax
import jax.numpy as jnp
from jax import lax

TOKENS = 16384
VOCAB_SIZE = 50304
MODEL_DIM = 768
MLP_WIDTH = 3072
RMS_EPS = 1e-6
ROW_BLOCK = math.gcd(TOKENS, 256)


def draw_token_ids(key):
    key_mix, key_low, key_all, key_first, key_last = jax.random.split(key, 5)
    choose_low = jax.random.randint(key_mix, (TOKENS,), 0, 4) == 0
    low_ids = jax.random.randint(key_low, (TOKENS,), 0, VOCAB_SIZE // 8)
    any_ids = jax.random.randint(key_all, (TOKENS,), 0, VOCAB_SIZE)
    token_ids = jnp.where(choose_low, low_ids, any_ids)
    first_pos = jax.random.randint(key_first, (), 0, TOKENS // 2)
    last_pos = jax.random.randint(key_last, (), TOKENS // 2, TOKENS)
    token_ids = token_ids.at[first_pos].set(0).at[last_pos].set(VOCAB_SIZE - 1)
    return token_ids.astype(jnp.int32)


def setup_inputs(seed: int = 0, part: int = 0) -> dict:
    base_key = jax.random.key(seed)
    key_ids = jax.random.fold_in(jax.random.fold_in(base_key, 1), part)
    key_table, key_gain, key_in, key_out = jax.random.split(jax.random.fold_in(base_key, 2), 4)
    embed_table = jax.random.normal(key_table, (VOCAB_SIZE, MODEL_DIM), jnp.float32)
    norm_gain = jax.random.uniform(key_gain, (MODEL_DIM,), jnp.float32, 0.5, 1.5)
    w_in = jax.random.normal(key_in, (MODEL_DIM, MLP_WIDTH), jnp.float32) * MODEL_DIM ** -0.5
    w_out = jax.random.normal(key_out, (MLP_WIDTH, MODEL_DIM), jnp.float32) * MLP_WIDTH ** -0.5
    return {
        "token_ids": draw_token_ids(key_ids),
        "embed_table": embed_table.astype(jnp.bfloat16),
        "norm_gain": norm_gain.astype(jnp.bfloat16),
        "w_in": w_in.astype(jnp.bfloat16),
        "w_out": w_out.astype(jnp.bfloat16),
    }


def block_forward(embed_rows, norm_gain, w_in, w_out):
    rows_f32 = embed_rows.astype(jnp.float32)
    inv_rms = lax.rsqrt(jnp.mean(rows_f32 * rows_f32, axis=-1, keepdims=True) + RMS_EPS)
    normed = (rows_f32 * inv_rms * norm_gain.astype(jnp.float32)).astype(jnp.bfloat16)
    pre_act = jnp.dot(normed, w_in, preferred_element_type=jnp.float32).astype(jnp.bfloat16)
    activated = jax.nn.gelu(pre_act.astype(jnp.float32), approximate=True).astype(jnp.bfloat16)
    mlp_sum = jnp.dot(activated, w_out, preferred_element_type=jnp.float32)
    return (rows_f32 + mlp_sum).astype(jnp.bfloat16)


def reference(token_ids, embed_table, norm_gain, w_in, w_out):
    embedded = jnp.take(embed_table, token_ids, axis=0)
    row_blocks = embedded.reshape(TOKENS // ROW_BLOCK, ROW_BLOCK, MODEL_DIM)
    outputs = lax.map(lambda row_blk: block_forward(row_blk, norm_gain, w_in, w_out), row_blocks)
    return outputs.reshape(TOKENS, MODEL_DIM)
```

```python
import functools
import math

import jax
import jax.numpy as jnp
from jax import lax
from jax.experimental import pallas as pl
from jax.experimental.pallas import tpu as pltpu
from jax.sharding import PartitionSpec as P

RMS_EPS = 1e-6
MESH = pl.DeviceIdType.MESH
CAP = 80
GROUP = 8
F32, BF16 = jnp.float32, jnp.bfloat16


def iota(shape, dim):
    return lax.broadcasted_iota(jnp.int32, shape, dim).astype(F32)


def kernel(n, side, cap, do_rows, do_mlp, *refs):
    refs = list(refs)
    take = lambda count: [refs.pop(0) for _ in range(count)]
    if do_rows:
        round_ref, ids_ref, table_ref = take(3)
    else:
        (x_in_ref,) = take(1)
    if do_mlp:
        gain_ref, w_ref = take(2)
    (out_ref,) = take(1)
    if do_rows and do_mlp:
        (count_ref,) = take(1)
    x_ref, acc_ref, send_sem = take(3)
    if do_rows:
        key_ref, local_ref, hot_ref, pack_ref, rows_ref, rows_sem = take(6)
        vocab, tokens = table_ref.shape[0], ids_ref.shape[1]
    if do_mlp:
        w_all, w1_ref, w2_ref, n_ref, w_sem, sib_sem = take(6)

    me = lax.axis_index("tp")
    y, x, core = me // (2 * side), (me // 2) % side, me % 2

    def device(dy, dx, dc=0):
        return (lax.rem(y + dy + side, side) * side + lax.rem(x + dx + side, side)) * 2 + lax.rem(core + dc, 2)

    sent = []

    def send(src, dst, recv_sem, target):
        copy = pltpu.make_async_remote_copy(
            src_ref=src, dst_ref=dst, send_sem=send_sem.at[len(sent)], recv_sem=recv_sem,
            device_id={"tp": target}, device_id_type=MESH)
        copy.start()
        sent.append(copy)

    def wait(ref, recv_sem):
        pltpu.make_async_remote_copy(
            src_ref=ref, dst_ref=ref, send_sem=send_sem.at[0], recv_sem=recv_sem,
            device_id={"tp": me}, device_id_type=MESH).wait_recv()

    barrier = pltpu.get_barrier_semaphore()

    def greet(k, carry):
        pl.semaphore_signal(barrier, inc=1, device_id={"tp": lax.rem(me + k, n)}, device_id_type=MESH)
        return carry

    lax.fori_loop(1, n, greet, 0)

    def piece(half, a, b, owner_core):
        dx, dy = (a, b) if half == 0 else (b, a)
        return w_all.at[lax.rem(y - dy + side, side), lax.rem(x - dx + side, side), owner_core, half]

    def along(half, first, step):
        return device(0, step) if (half == 0) == first else device(step, 0)

    def spot(a, b):
        return a * side + b

    def second_axis(half, a, src, dst):
        send(src, dst, w_sem.at[half, 0, spot(a, 1)], along(half, False, 1))
        send(src, dst, w_sem.at[half, 0, spot(a, 3)], along(half, False, -1))

    def own_weights(half):
        src, dst = w_ref.at[half], piece(half, 0, 0, core)
        send(src, dst, w_sem.at[half, 0, spot(1, 0)], along(half, True, 1))
        send(src, dst, w_sem.at[half, 0, spot(3, 0)], along(half, True, -1))
        second_axis(half, 0, src, dst)
        send(src, dst, sib_sem.at[half, spot(0, 0)], device(0, 0, 1))

    def got(half, a, b):
        here = piece(half, a, b, core)
        if b == 2 or (a, b) == (2, 0):
            for part in range(2):
                wait(here.at[part], w_sem.at[half, part, spot(a, b)])
        else:
            wait(here, w_sem.at[half, 0, spot(a, b)])
        if b == 0:
            if a == 1:
                send(here.at[0], here.at[0], w_sem.at[half, 0, spot(2, 0)], along(half, True, 1))
            if a == 3:
                send(here.at[1], here.at[1], w_sem.at[half, 1, spot(2, 0)], along(half, True, -1))
            second_axis(half, a, here, here)
        if b == 1:
            send(here.at[0], here.at[0], w_sem.at[half, 0, spot(a, 2)], along(half, False, 1))
        if b == 3:
            send(here.at[1], here.at[1], w_sem.at[half, 1, spot(a, 2)], along(half, False, -1))
        send(here, here, sib_sem.at[half, spot(a, b)], device(0, 0, 1))

    def sibling(b):
        for half in range(2):
            for a in range(side):
                wait(piece(half, a, b, 1 - core), sib_sem.at[half, spot(a, b)])

    if do_rows:
        ids = ids_ref[...].astype(F32)
        local = ids - (me * vocab).astype(F32)
        owned = (local >= 0) & (local < vocab)
        before = (iota((tokens, tokens), 0) < iota((tokens, tokens), 1)).astype(BF16)
        rank = jnp.dot(jnp.where(owned, 1.0, 0.0).astype(BF16), before, preferred_element_type=F32)
        first = (round_ref[0] * cap).astype(F32)
        key_ref[...] = jnp.where(owned, rank - first, -1.0)
        local_ref[...] = local + 1.0

    if do_mlp:
        w_all[y, x, core] = w_ref[...]

    pl.semaphore_wait(barrier, n - 1)

    if do_mlp:
        own_weights(0)
        own_weights(1)

    if do_rows:
        def pack(group):
            for j in range(GROUP):
                dest = lax.rem(me + group * GROUP + j, n)
                key, val = key_ref[pl.ds(dest, 1), :], local_ref[pl.ds(dest, 1), :]
                row = jnp.sum(jnp.where(key == iota((cap, tokens), 0), val, 0.0), axis=1, keepdims=True) - 1.0
                hot_ref[j] = (row == iota((cap, vocab), 1)).astype(BF16)
            rows = jnp.dot(hot_ref[...].reshape(GROUP * cap, vocab), table_ref[...], preferred_element_type=F32)
            pack_ref[pl.ds(group * GROUP, GROUP)] = rows.astype(BF16).reshape(GROUP, cap, -1)

        def send_rows(group):
            for k in range(max(1, group * GROUP), (group + 1) * GROUP):
                send(pack_ref.at[k], rows_ref.at[me], rows_sem.at[k], lax.rem(me + k, n))

        for group in range(n // GROUP):
            pack(group)
            if group == 0:
                rows_ref[me] = pack_ref[0]
            else:
                send_rows(group - 1)
            if do_mlp and group == 1:
                for half in range(2):
                    got(half, 1, 0)
                    got(half, 3, 0)
            if do_mlp and group == 2:
                for half in range(2):
                    got(half, 0, 1)
                    got(half, 0, 3)
        if do_mlp:
            for half in range(2):
                got(half, 2, 0)
        send_rows(n // GROUP - 1)

        mine = ids_ref[pl.ds(me, 1), :].astype(F32)
        owner_row = jnp.floor((mine + 0.5) * (1.0 / vocab))
        p_col, p_row = iota((tokens, tokens), 0), iota((tokens, tokens), 1)
        owner_col = jnp.sum(jnp.where(p_col == p_row, owner_row, 0.0), axis=1, keepdims=True)
        place = jnp.sum(jnp.where((owner_col == owner_row) & (p_row < p_col), 1.0, 0.0), axis=1, keepdims=True)
        place = place - first
        slot = jnp.where((place >= 0) & (place < cap), owner_col * cap + place, -1.0)
        if do_mlp:
            owner_all = jnp.floor((ids + 0.5) * (1.0 / vocab))
            most = jnp.zeros((n, 1), F32)
            for owner in range(n):
                most = jnp.maximum(most, jnp.sum(jnp.where(owner_all == owner, 1.0, 0.0), axis=1, keepdims=True))
            count_ref[...] = jnp.broadcast_to(jnp.max(most, axis=0, keepdims=True), count_ref.shape)

        for k in range(1, n):
            wait(rows_ref.at[lax.rem(me - k + n, n)], rows_sem.at[k])
        for group in range(n // GROUP):
            hot = (slot - (group * GROUP * cap) == iota((tokens, GROUP * cap), 1)).astype(BF16)
            part = jnp.dot(hot, rows_ref[pl.ds(group * GROUP, GROUP)].reshape(GROUP * cap, -1),
                           preferred_element_type=F32)
            if group == 0:
                acc_ref[...] = part
            else:
                acc_ref[...] += part
        x_ref[...] = acc_ref[...].astype(BF16)
    else:
        x_ref[...] = x_in_ref[...]
        for half in range(2):
            got(half, 1, 0)
            got(half, 3, 0)
            got(half, 0, 1)
            got(half, 0, 3)
            got(half, 2, 0)

    if do_mlp:
        rows = x_ref[...].astype(F32)
        inv_rms = lax.rsqrt(jnp.mean(rows * rows, axis=-1, keepdims=True) + RMS_EPS)
        n_ref[...] = (rows * inv_rms * gain_ref[...].astype(F32)).astype(BF16)
        acc_ref[...] = jnp.zeros_like(acc_ref)
        span = w1_ref.shape[0] // 2
        tile = min(256, acc_ref.shape[0])

        def mlp(b):
            row, col = lax.rem(y - b + side, side), lax.rem(x - b + side, side)
            for part, dst in enumerate((w1_ref, w2_ref)):
                dst[:span] = w_all[row, :, :, 0, part].reshape(span, -1)
                dst[span:] = w_all[:, col, :, 1, part].reshape(span, -1)

            def step(t, carry):
                at = pl.ds(pl.multiple_of(t * tile, tile), tile)
                u = lax.dot_general(n_ref[at, :], w1_ref[...], (((1,), (1,)), ((), ())), preferred_element_type=F32)
                h = jax.nn.gelu(u.astype(BF16).astype(F32), approximate=True).astype(BF16)
                acc_ref[at, :] += jnp.dot(h, w2_ref[...], preferred_element_type=F32)
                return carry

            lax.fori_loop(0, acc_ref.shape[0] // tile, step, 0)

        sibling(0)
        mlp(0)
        for a in (1, 3, 2):
            for half in range(2):
                got(half, a, 1)
                got(half, a, 3)
        sibling(1)
        mlp(1)
        for a in (0, 1, 3, 2):
            for half in range(2):
                got(half, a, 2)
        sibling(3)
        mlp(3)
        sibling(2)
        mlp(2)
        out_ref[...] = (x_ref[...].astype(F32) + acc_ref[...]).astype(BF16)
    else:
        out_ref[...] = x_ref[...]
    for copy in sent:
        copy.wait_send()


def call(n, side, cap, do_rows, do_mlp, tokens, dim, vocab, share):
    vmem, dma = pltpu.VMEM, pltpu.SemaphoreType.DMA
    spec = pl.BlockSpec(memory_space=pltpu.VMEM)
    in_specs, out_shape, sends = [], [jax.ShapeDtypeStruct((tokens, dim), BF16)], 0
    scratch = []
    if do_rows:
        in_specs += [pl.BlockSpec(memory_space=pltpu.SMEM), spec, spec]
        scratch += [vmem((n, tokens), F32), vmem((n, tokens), F32), vmem((GROUP, cap, vocab), BF16),
                    vmem((n, cap, dim), BF16), vmem((n, cap, dim), BF16), dma((n,))]
        sends += n - 1
    else:
        in_specs += [spec]
    if do_mlp:
        in_specs += [spec, spec]
        scratch += [vmem((side, side, 2, 2, 2, share // 2, dim), BF16), vmem((n * share // side, dim), BF16),
                    vmem((n * share // side, dim), BF16), vmem((tokens, dim), BF16),
                    dma((2, 2, side * side)), dma((2, side * side))]
        sends += 2 * (4 + 16 + side * side)
    if do_rows and do_mlp:
        out_shape += [jax.ShapeDtypeStruct((8, 128), F32)]
    scratch = [vmem((tokens, dim), BF16), vmem((tokens, dim), F32), dma((sends,))] + scratch
    return pl.pallas_call(
        functools.partial(kernel, n, side, cap, do_rows, do_mlp),
        out_shape=out_shape,
        in_specs=in_specs,
        out_specs=[spec] * len(out_shape),
        scratch_shapes=scratch,
        compiler_params=pltpu.CompilerParams(
            collective_id=2 * do_rows + do_mlp, has_side_effects=True, vmem_limit_bytes=60 * 2**20),
    )


def solution(mesh):
    n = mesh.shape["tp"]
    side = math.isqrt(n // 2)

    def device_step(token_ids, table_shard, norm_gain, w_in_shard, w_out_shard):
        vocab, dim = table_shard.shape
        share = w_out_shard.shape[0]
        tokens = token_ids.shape[0] // n
        make = functools.partial(call, n, side, CAP, tokens=tokens, dim=dim, vocab=vocab, share=share)
        ids = token_ids.reshape(n, tokens)
        gain = norm_gain.reshape(1, dim)
        weights = jnp.stack([w_in_shard.T.reshape(2, share // 2, dim), w_out_shard.reshape(2, share // 2, dim)], axis=1)
        out, most = make(True, True)(jnp.zeros((1,), jnp.int32), ids, table_shard, gain, weights)
        rounds = lax.div(most[0, 0].astype(jnp.int32) + CAP - 1, CAP)

        def more_rounds():
            def one(carry):
                r, rows = carry
                (new,) = make(True, False)(r.reshape(1), ids, table_shard)
                return r + 1, rows + new

            _, rows = lax.while_loop(lambda carry: carry[0] < rounds, one,
                                     (jnp.int32(0), jnp.zeros((tokens, dim), BF16)))
            return make(False, True)(rows, gain, weights)[0]

        return lax.cond(rounds > 1, more_rounds, lambda: out)

    return jax.shard_map(
        device_step,
        mesh=mesh,
        in_specs=(P("dp"), P("tp", None), P(), P(None, "tp"), P("tp", None)),
        out_specs=P(("dp", "tp"), None),
        check_vma=False,
    )
```

```python
import functools
import math

import jax
import jax.numpy as jnp
from jax import lax
from jax.experimental import pallas as pl
from jax.experimental.pallas import tpu as pltpu
from jax.sharding import PartitionSpec as P

RMS_EPS = 1e-6
MESH = pl.DeviceIdType.MESH
TURN_CAP, LAST_CAP = 224, 272
CAP, GROUP = 64, 8
F32, BF16 = jnp.float32, jnp.bfloat16


def iota(shape, dim):
    return lax.broadcasted_iota(jnp.int32, shape, dim).astype(F32)


def ones(mask):
    return jnp.where(mask, 1.0, 0.0)


def count_before(mask):
    tokens = mask.shape[1]
    before = ones(iota((tokens, tokens), 0) < iota((tokens, tokens), 1)).astype(BF16)
    return jnp.dot(mask.astype(BF16), before, preferred_element_type=F32)


def as_column(row):
    tokens = row.shape[1]
    return jnp.sum(jnp.where(iota((tokens, tokens), 0) == iota((tokens, tokens), 1), row, 0.0), axis=1, keepdims=True)


def place_among(kind):
    column = as_column(kind)
    tokens = kind.shape[1]
    same = (column == kind) & (iota((tokens, tokens), 1) < iota((tokens, tokens), 0))
    return column, jnp.sum(ones(same), axis=1, keepdims=True)


def coords(device, side):
    y = jnp.floor((device + 0.5) * (0.5 / side))
    x = jnp.floor((device - y * (2 * side) + 0.5) * 0.5)
    return y, x, device - y * (2 * side) - x * 2


def owner_of(ids, vocab):
    return jnp.floor((ids + 0.5) * (1.0 / vocab))


def greet_all(n, me):
    def greet(k, carry):
        pl.semaphore_signal(pltpu.get_barrier_semaphore(), inc=1, device_id={"tp": lax.rem(me + k, n)},
                            device_id_type=MESH)
        return carry

    lax.fori_loop(1, n, greet, 0)


def remote(src, dst, send_sem, recv_sem, target):
    return pltpu.make_async_remote_copy(src_ref=src, dst_ref=dst, send_sem=send_sem, recv_sem=recv_sem,
                                        device_id={"tp": target}, device_id_type=MESH)


def rows_kernel(n, cap, round_ref, ids_ref, table_ref, out_ref, key_ref, local_ref, hot_ref, pack_ref, rows_ref, acc_ref,
                send_sem, rows_sem):
    vocab, tokens = table_ref.shape[0], ids_ref.shape[1]
    me = lax.axis_index("tp")
    greet_all(n, me)
    local = ids_ref[...].astype(F32) - (me * vocab).astype(F32)
    owned = (local >= 0) & (local < vocab)
    first = (round_ref[0] * cap).astype(F32)
    key_ref[...] = jnp.where(owned, count_before(ones(owned)) - first, -1.0)
    local_ref[...] = local + 1.0
    pl.semaphore_wait(pltpu.get_barrier_semaphore(), n - 1)

    def pack(group, carry):
        def fill(j, carry):
            dest = lax.rem(me + group * GROUP + j, n)
            key, val = key_ref[pl.ds(dest, 1), :], local_ref[pl.ds(dest, 1), :]
            row = jnp.sum(jnp.where(key == iota((cap, tokens), 0), val, 0.0), axis=1, keepdims=True) - 1.0
            hot_ref[j] = (row == iota((cap, vocab), 1)).astype(BF16)
            return carry

        lax.fori_loop(0, GROUP, fill, 0)
        rows = jnp.dot(hot_ref[...].reshape(GROUP * cap, vocab), table_ref[...], preferred_element_type=F32)
        pack_ref[pl.ds(group * GROUP, GROUP)] = rows.astype(BF16).reshape(GROUP, cap, -1)
        return carry

    lax.fori_loop(0, n // GROUP, pack, 0)

    def pair(k, source):
        return remote(pack_ref.at[k], rows_ref.at[source], send_sem.at[k], rows_sem.at[k], lax.rem(me + k, n))

    def start(k, carry):
        pair(k, me).start()
        return carry

    lax.fori_loop(1, n, start, 0)
    rows_ref[me] = pack_ref[0]
    owner, place = place_among(owner_of(ids_ref[pl.ds(me, 1), :].astype(F32), vocab))
    place = place - first
    slot = jnp.where((place >= 0) & (place < cap), owner * cap + place, -1.0)

    def finish(k, carry):
        pair(k, lax.rem(me - k + n, n)).wait_recv()
        pair(k, me).wait_send()
        return carry

    lax.fori_loop(1, n, finish, 0)
    acc_ref[...] = jnp.zeros_like(acc_ref)

    def unpack(group, carry):
        hot = (slot - (group * (GROUP * cap)).astype(F32) == iota((tokens, GROUP * cap), 1)).astype(BF16)
        acc_ref[...] += jnp.dot(hot, rows_ref[pl.ds(group * GROUP, GROUP)].reshape(GROUP * cap, -1),
                                preferred_element_type=F32)
        return carry

    lax.fori_loop(0, n // GROUP, unpack, 0)
    out_ref[...] = acc_ref[...].astype(BF16)


def block_kernel(n, side, do_rows, *refs):
    refs = list(refs)
    take = lambda count: [refs.pop(0) for _ in range(count)]
    if do_rows:
        ids_ref, table_ref = take(2)
    else:
        (x_in_ref,) = take(1)
    gain_ref, w_ref, out_ref = take(3)
    if do_rows:
        (count_ref,) = take(1)
    x_ref, acc_ref, w_all, w1_ref, w2_ref, n_ref, send_sem, w_sem, sib_sem = take(9)
    if do_rows:
        key_ref, local_ref, owner_ref, hot_ref, pack_ref, mid_ref, turn_ref, last_ref, rows_ref, mid_sem, rows_sem = take(11)
        vocab, tokens = table_ref.shape[0], ids_ref.shape[1]

    me = lax.axis_index("tp")
    y, x, core = me // (2 * side), (me // 2) % side, me % 2

    def device(dy, dx, dc=0):
        return (lax.rem(y + dy + side, side) * side + lax.rem(x + dx + side, side)) * 2 + lax.rem(core + dc, 2)

    sent = []

    def send(src, dst, recv_sem, target):
        copy = remote(src, dst, send_sem.at[len(sent)], recv_sem, target)
        copy.start()
        sent.append(copy)

    def wait(ref, recv_sem):
        remote(ref, ref, send_sem.at[0], recv_sem, me).wait_recv()

    greet_all(n, me)

    def piece(half, a, b, owner_core):
        dx, dy = (a, b) if half == 0 else (b, a)
        return w_all.at[lax.rem(y - dy + side, side), lax.rem(x - dx + side, side), owner_core, half]

    def along(half, first, step):
        return device(0, step) if (half == 0) == first else device(step, 0)

    def spot(a, b):
        return a * side + b

    def second_axis(half, a, src, dst):
        send(src, dst, w_sem.at[half, 0, spot(a, 1)], along(half, False, 1))
        send(src, dst, w_sem.at[half, 0, spot(a, 3)], along(half, False, -1))

    def own_weights(half):
        src, dst = w_ref.at[half], piece(half, 0, 0, core)
        send(src, dst, w_sem.at[half, 0, spot(1, 0)], along(half, True, 1))
        send(src, dst, w_sem.at[half, 0, spot(3, 0)], along(half, True, -1))
        second_axis(half, 0, src, dst)
        send(src, dst, sib_sem.at[half, spot(0, 0)], device(0, 0, 1))

    def got(half, a, b):
        here = piece(half, a, b, core)
        if b == 2 or (a, b) == (2, 0):
            for part in range(2):
                wait(here.at[part], w_sem.at[half, part, spot(a, b)])
        else:
            wait(here, w_sem.at[half, 0, spot(a, b)])
        if b == 0:
            if a == 1:
                send(here.at[0], here.at[0], w_sem.at[half, 0, spot(2, 0)], along(half, True, 1))
            if a == 3:
                send(here.at[1], here.at[1], w_sem.at[half, 1, spot(2, 0)], along(half, True, -1))
            second_axis(half, a, here, here)
        if b == 1:
            send(here.at[0], here.at[0], w_sem.at[half, 0, spot(a, 2)], along(half, False, 1))
        if b == 3:
            send(here.at[1], here.at[1], w_sem.at[half, 1, spot(a, 2)], along(half, False, -1))
        send(here, here, sib_sem.at[half, spot(a, b)], device(0, 0, 1))

    def got_all(*spots):
        for a, b in spots:
            for half in range(2):
                got(half, a, b)

    def sibling(b):
        for half in range(2):
            for a in range(side):
                wait(piece(half, a, b, 1 - core), sib_sem.at[half, spot(a, b)])

    def line_device(half, line, i):
        in_x, in_y = (i * side + line) * 2, (line * side + i) * 2 + 1
        return in_x if isinstance(half, int) and half == 0 else in_y if isinstance(half, int) else jnp.where(half == 0, in_x, in_y)

    w_all[y, x, core] = w_ref[...]
    if do_rows:
        ids = ids_ref[...].astype(F32)
        local = ids - (me * vocab).astype(F32)
        owned = ones((local >= 0) & (local < vocab))
        dy, dx, dc = coords(iota((n, n), 0), side)
        ey, ex, ec = coords(iota((n, n), 1), side)
        same_line = ones(dc == ec) * jnp.where(dc == 0, ones(dx == ex), ones(dy == ey))
        earlier = same_line * jnp.where(dc == 0, ones(ey < dy), ones(ex < dx))
        in_line = jnp.dot(earlier.astype(BF16), owned.astype(BF16), preferred_element_type=F32)
        rank = count_before(owned) + jnp.sum(in_line, axis=1, keepdims=True)
        key_ref[...] = jnp.where(owned > 0, rank, -1.0)
        local_ref[...] = local + 1.0
        owner_ref[...] = owner_of(ids, vocab)

    pl.semaphore_wait(pltpu.get_barrier_semaphore(), n - 1)
    own_weights(0)
    own_weights(1)

    if do_rows:
        first_axis = jnp.where(core == 0, x, y)
        last_axis = jnp.where(core == 0, y, x)
        turn_cap, last_cap = mid_ref.shape[1], rows_ref.shape[1]

        def pack(half, line):
            row = jnp.zeros((turn_cap, 1), F32)
            for i in range(side):
                dest = line_device(half, line, i)
                key, val = key_ref[pl.ds(dest, 1), :], local_ref[pl.ds(dest, 1), :]
                row += jnp.sum(jnp.where(key == iota((turn_cap, tokens), 0), val, 0.0), axis=1, keepdims=True)
            hot_ref[...] = (row - 1.0 == iota((turn_cap, vocab), 1)).astype(BF16)
            return jnp.dot(hot_ref[...], table_ref[...], preferred_element_type=F32).astype(BF16)

        todo = []
        for step in (1, 3, 2):
            for half in range(2):
                at = len(todo)
                here = x if half == 0 else y
                pack_ref[at] = pack(half, lax.rem(here + step, side))
                target = (y * side + lax.rem(x + step, side)) * 2 if half == 0 else (lax.rem(y + step, side) * side + x) * 2 + 1
                todo.append((at, here * 2 + core, mid_sem.at[step * 2 + core], target))
                if at > 0:
                    at, j, sem, target = todo[at - 1]
                    send(pack_ref.at[at], mid_ref.at[j], sem, target)
        at = len(todo)
        pack_ref[at] = pack(1 - core, last_axis)
        send(pack_ref.at[at - 1], mid_ref.at[todo[-1][1]], todo[-1][2], todo[-1][3])
        mid_ref[first_axis * 2 + core] = pack(core, first_axis)
        send(pack_ref.at[at], mid_ref.at[last_axis * 2 + core], mid_sem.at[0], device(0, 0, 1))
        got_all((1, 0), (3, 0))

        j = lax.broadcasted_iota(jnp.int32, (2 * side, 1), 0)
        source = jnp.where(core == 0, y * (2 * side) + j, (j >> 1) * (2 * side) + x * 2 + (j & 1)).astype(F32)
        for i in range(side):
            mine = owner_ref[pl.ds(line_device(core, first_axis, i), 1), :]
            turn_ref[i * 2 * side:(i + 1) * 2 * side, :] = ones(mine == source)
        from_source = turn_ref[...]
        in_block = count_before(from_source)
        r, c = iota((n, n), 0), iota((n, n), 1)
        (ri, _, _), (ci, _, _) = coords(r, side), coords(c, side)
        earlier = (r - ri * (2 * side) == c - ci * (2 * side)) & (ci < ri)
        in_line = jnp.dot(ones(earlier).astype(BF16), from_source.astype(BF16), preferred_element_type=F32)
        slot = in_block + jnp.sum(in_line, axis=1, keepdims=True) + 1.0
        for i in range(side):
            part = slice(i * 2 * side, (i + 1) * 2 * side)
            mask = from_source[part]
            at = jnp.sum(mask * (slot[part] + j.astype(F32) * turn_cap), axis=0, keepdims=True)
            rank = jnp.sum(in_block[part], axis=0, keepdims=True)
            key_ref[i:i + 1, :] = jnp.where(at > 0, rank, -1.0)
            local_ref[i:i + 1, :] = at

        own_y, own_x, _ = coords(owner_ref[pl.ds(me, 1), :], side)
        via, place = place_among(jnp.where(core == 0, own_y, own_x))
        slot = via * last_cap + place

        def count(owner, counts):
            here = jnp.sum(ones(owner_ref[...] == owner.astype(F32)), axis=1, keepdims=True)
            return jnp.where(iota(counts.shape, 1) == owner.astype(F32), here, counts)

        counts = lax.fori_loop(0, n, count, jnp.zeros((n, 128), F32))
        exact = functools.partial(jnp.dot, precision=lax.Precision.HIGHEST, preferred_element_type=F32)
        bundles = exact(same_line, counts)
        oy, ox, _ = coords(iota((128, 128), 0), side)
        g = iota((128, 128), 1)
        blocks = exact(counts, ones((oy == g) | ((oy < side) & (ox == g - side))))
        lane = iota((n, 128), 1)
        dest_core = coords(iota((n, 128), 0), side)[2]
        counted = jnp.where(dest_core == 0, ones(lane < side), ones((lane >= side) & (lane < 2 * side)))
        over = ones(bundles > turn_cap) + counted * ones(blocks > last_cap)
        worst = lambda value: jnp.max(jnp.max(value, axis=0, keepdims=True), axis=1, keepdims=True)
        count_ref[0:1, :] = jnp.broadcast_to(worst(over), (1, 128))
        count_ref[1:2, :] = jnp.broadcast_to(worst(counts), (1, 128))

        wait(mid_ref.at[first_axis * 2 + 1 - core], mid_sem.at[0])
        for step in (1, 3, 2):
            for sc in range(2):
                wait(mid_ref.at[lax.rem(first_axis - step + side, side) * 2 + sc], mid_sem.at[step * 2 + sc])

        def turn(step):
            i = lax.rem(last_axis + step, side)
            key, val = key_ref[pl.ds(i, 1), :], local_ref[pl.ds(i, 1), :]
            row = jnp.sum(jnp.where(key == iota((last_cap, tokens), 0), val, 0.0), axis=1, keepdims=True) - 1.0
            hot = (row == iota((last_cap, 2 * side * turn_cap), 1)).astype(BF16)
            return jnp.dot(hot, mid_ref[...].reshape(2 * side * turn_cap, -1), preferred_element_type=F32).astype(BF16)

        def send_turn(step):
            send(last_ref.at[step], rows_ref.at[last_axis], rows_sem.at[step],
                 jnp.where(core == 0, device(step, 0), device(0, step)))

        last_ref[1] = turn(1)
        last_ref[3] = turn(3)
        send_turn(1)
        last_ref[2] = turn(2)
        send_turn(3)
        rows_ref[last_axis] = turn(0)
        send_turn(2)
        got_all((2, 0), (0, 1), (0, 3), (1, 1), (1, 3), (3, 1), (3, 3))

        for step in (1, 3, 2):
            wait(rows_ref.at[lax.rem(last_axis - step + side, side)], rows_sem.at[step])
        hot = (slot == iota((tokens, side * last_cap), 1)).astype(BF16)
        x_ref[...] = jnp.dot(hot, rows_ref[...].reshape(side * last_cap, -1), preferred_element_type=F32).astype(BF16)
    else:
        x_ref[...] = x_in_ref[...]
        got_all((1, 0), (3, 0), (2, 0), (0, 1), (0, 3), (1, 1), (1, 3), (3, 1), (3, 3))

    rows = x_ref[...].astype(F32)
    inv_rms = lax.rsqrt(jnp.mean(rows * rows, axis=-1, keepdims=True) + RMS_EPS)
    n_ref[...] = (rows * inv_rms * gain_ref[...].astype(F32)).astype(BF16)
    acc_ref[...] = jnp.zeros_like(acc_ref)
    span = w1_ref.shape[0] // 2
    tile = min(256, acc_ref.shape[0])

    def mlp(b):
        row, col = lax.rem(y - b + side, side), lax.rem(x - b + side, side)
        for part, dst in enumerate((w1_ref, w2_ref)):
            dst[:span] = w_all[row, :, :, 0, part].reshape(span, -1)
            dst[span:] = w_all[:, col, :, 1, part].reshape(span, -1)

        def step(t, carry):
            at = pl.ds(pl.multiple_of(t * tile, tile), tile)
            u = lax.dot_general(n_ref[at, :], w1_ref[...], (((1,), (1,)), ((), ())), preferred_element_type=F32)
            h = jax.nn.gelu(u.astype(BF16).astype(F32), approximate=True).astype(BF16)
            acc_ref[at, :] += jnp.dot(h, w2_ref[...], preferred_element_type=F32)
            return carry

        lax.fori_loop(0, acc_ref.shape[0] // tile, step, 0)

    if do_rows:
        sibling(0)
        mlp(0)
        got_all((2, 1), (2, 3))
        sibling(1)
        mlp(1)
        got_all((0, 2), (1, 2), (3, 2))
        sibling(3)
        mlp(3)
        got_all((2, 2))
        sibling(2)
        mlp(2)
    else:
        got_all((2, 1), (2, 3), (0, 2), (1, 2), (3, 2), (2, 2))
        for b in range(side):
            sibling(b)

        def every(b, carry):
            mlp(b)
            return carry

        lax.fori_loop(0, side, every, 0)
    out_ref[...] = (x_ref[...].astype(F32) + acc_ref[...]).astype(BF16)
    for copy in sent:
        copy.wait_send()


def params(collective_id):
    return pltpu.CompilerParams(collective_id=collective_id, has_side_effects=True, vmem_limit_bytes=60 * 2**20)


def rows_call(n, tokens, dim, vocab):
    vmem, dma = pltpu.VMEM, pltpu.SemaphoreType.DMA
    spec = pl.BlockSpec(memory_space=pltpu.VMEM)
    return pl.pallas_call(
        functools.partial(rows_kernel, n, CAP),
        out_shape=jax.ShapeDtypeStruct((tokens, dim), BF16),
        in_specs=[pl.BlockSpec(memory_space=pltpu.SMEM), spec, spec],
        out_specs=spec,
        scratch_shapes=[vmem((n, tokens), F32), vmem((n, tokens), F32), vmem((GROUP, CAP, vocab), BF16),
                        vmem((n, CAP, dim), BF16), vmem((n, CAP, dim), BF16), vmem((tokens, dim), F32),
                        dma((n,)), dma((n,))],
        compiler_params=params(0))


def block_call(n, side, do_rows, tokens, dim, vocab, share):
    vmem, dma = pltpu.VMEM, pltpu.SemaphoreType.DMA
    spec = pl.BlockSpec(memory_space=pltpu.VMEM)
    out_shape = [jax.ShapeDtypeStruct((tokens, dim), BF16)]
    sends = 2 * (4 + 16 + side * side) + (7 + 3 if do_rows else 0)
    scratch = [vmem((tokens, dim), BF16), vmem((tokens, dim), F32),
               vmem((side, side, 2, 2, 2, share // 2, dim), BF16), vmem((n * share // side, dim), BF16),
               vmem((n * share // side, dim), BF16), vmem((tokens, dim), BF16),
               dma((sends,)), dma((2, 2, side * side)), dma((2, side * side))]
    if do_rows:
        out_shape += [jax.ShapeDtypeStruct((2, 128), F32)]
        scratch += [vmem((n, tokens), F32)] * 3 + [
            vmem((TURN_CAP, vocab), BF16), vmem((2 * side - 1, TURN_CAP, dim), BF16), vmem((2 * side, TURN_CAP, dim), BF16),
            vmem((n, tokens), F32), vmem((side, LAST_CAP, dim), BF16), vmem((side, LAST_CAP, dim), BF16),
            dma((2 * side,)), dma((side,))]
    return pl.pallas_call(
        functools.partial(block_kernel, n, side, do_rows),
        out_shape=out_shape,
        in_specs=[spec] * (4 if do_rows else 3),
        out_specs=[spec] * len(out_shape),
        scratch_shapes=scratch,
        compiler_params=params(1 + do_rows))


def solution(mesh):
    n = mesh.shape["tp"]
    side = math.isqrt(n // 2)

    def device_step(token_ids, table_shard, norm_gain, w_in_shard, w_out_shard):
        vocab, dim = table_shard.shape
        share = w_out_shard.shape[0]
        tokens = token_ids.shape[0] // n
        ids = token_ids.reshape(n, tokens)
        gain = norm_gain.reshape(1, dim)
        weights = jnp.stack([w_in_shard.T.reshape(2, share // 2, dim), w_out_shard.reshape(2, share // 2, dim)], axis=1)
        out, counts = block_call(n, side, True, tokens, dim, vocab, share)(ids, table_shard, gain, weights)

        def in_rounds():
            rounds = lax.div(counts[1, 0].astype(jnp.int32) + CAP - 1, CAP)

            def one(carry):
                r, rows = carry
                return r + 1, rows + rows_call(n, tokens, dim, vocab)(r.reshape(1), ids, table_shard)

            _, rows = lax.while_loop(lambda carry: carry[0] < rounds, one,
                                     (jnp.int32(0), jnp.zeros((tokens, dim), BF16)))
            return block_call(n, side, False, tokens, dim, vocab, share)(rows, gain, weights)[0]

        return lax.cond(counts[0, 0] > 0, in_rounds, lambda: out)

    return jax.shard_map(
        device_step,
        mesh=mesh,
        in_specs=(P("dp"), P("tp", None), P(), P(None, "tp"), P("tp", None)),
        out_specs=P(("dp", "tp"), None),
        check_vma=False,
    )
```

```python
import functools
import math

import jax
import jax.numpy as jnp
from jax import lax
from jax.experimental import pallas as pl
from jax.experimental.pallas import tpu as pltpu
from jax.sharding import PartitionSpec as P

RMS_EPS = 1e-6
MESH = pl.DeviceIdType.MESH
TURN_CAP, LAST_CAP = 224, 272
CAP, GROUP = 64, 8
VMEM_LIMIT = 44 * 2**20
GELU_SCALE = math.sqrt(2.0 / math.pi)
F32, BF16 = jnp.float32, jnp.bfloat16


def iota(shape, dim):
    return lax.broadcasted_iota(jnp.int32, shape, dim).astype(F32)


def ones(mask):
    return jnp.where(mask, 1.0, 0.0)


def count_before(mask):
    tokens = mask.shape[1]
    before = ones(iota((tokens, tokens), 0) < iota((tokens, tokens), 1)).astype(BF16)
    return jnp.dot(mask.astype(BF16), before, preferred_element_type=F32)


def as_column(row):
    tokens = row.shape[1]
    return jnp.sum(jnp.where(iota((tokens, tokens), 0) == iota((tokens, tokens), 1), row, 0.0), axis=1, keepdims=True)


def place_among(kind):
    column = as_column(kind)
    tokens = kind.shape[1]
    same = (column == kind) & (iota((tokens, tokens), 1) < iota((tokens, tokens), 0))
    return column, jnp.sum(ones(same), axis=1, keepdims=True)


def coords(device, side):
    y = jnp.floor((device + 0.5) * (0.5 / side))
    x = jnp.floor((device - y * (2 * side) + 0.5) * 0.5)
    return y, x, device - y * (2 * side) - x * 2


def owner_of(ids, vocab):
    return jnp.floor((ids + 0.5) * (1.0 / vocab))


def gelu(z):
    return (0.5 * z) * (1.0 + jnp.tanh(z * (GELU_SCALE + GELU_SCALE * 0.044715 * (z * z))))


def by_destination(ids_ref, n):
    each = ids_ref.shape[0] // n
    return jnp.concatenate([ids_ref[pl.ds(j, n, stride=each), :] for j in range(each)], axis=1).astype(F32)


def greet_all(n, me):
    def greet(k, carry):
        pl.semaphore_signal(pltpu.get_barrier_semaphore(), inc=1, device_id={"tp": lax.rem(me + k, n)},
                            device_id_type=MESH)
        return carry

    lax.fori_loop(1, n, greet, 0)


def remote(src, dst, send_sem, recv_sem, target):
    return pltpu.make_async_remote_copy(src_ref=src, dst_ref=dst, send_sem=send_sem, recv_sem=recv_sem,
                                        device_id={"tp": target}, device_id_type=MESH)


def rows_kernel(n, cap, round_ref, ids_ref, table_ref, out_ref, key_ref, local_ref, hot_ref, pack_ref, rows_ref, acc_ref,
                send_sem, rows_sem):
    vocab, tokens = table_ref.shape[0], ids_ref.shape[1]
    me = lax.axis_index("tp")
    greet_all(n, me)
    local = ids_ref[...].astype(F32) - (me * vocab).astype(F32)
    owned = (local >= 0) & (local < vocab)
    first = (round_ref[0] * cap).astype(F32)
    key_ref[...] = jnp.where(owned, count_before(ones(owned)) - first, -1.0)
    local_ref[...] = local + 1.0
    pl.semaphore_wait(pltpu.get_barrier_semaphore(), n - 1)

    def pack(group, carry):
        def fill(j, carry):
            dest = lax.rem(me + group * GROUP + j, n)
            key, val = key_ref[pl.ds(dest, 1), :], local_ref[pl.ds(dest, 1), :]
            row = jnp.sum(jnp.where(key == iota((cap, tokens), 0), val, 0.0), axis=1, keepdims=True) - 1.0
            hot_ref[j] = (row == iota((cap, vocab), 1)).astype(BF16)
            return carry

        lax.fori_loop(0, GROUP, fill, 0)
        rows = jnp.dot(hot_ref[...].reshape(GROUP * cap, vocab), table_ref[...], preferred_element_type=F32)
        pack_ref[pl.ds(group * GROUP, GROUP)] = rows.astype(BF16).reshape(GROUP, cap, -1)
        return carry

    lax.fori_loop(0, n // GROUP, pack, 0)

    def pair(k, source):
        return remote(pack_ref.at[k], rows_ref.at[source], send_sem.at[k], rows_sem.at[k], lax.rem(me + k, n))

    def start(k, carry):
        pair(k, me).start()
        return carry

    lax.fori_loop(1, n, start, 0)
    rows_ref[me] = pack_ref[0]
    owner, place = place_among(owner_of(ids_ref[pl.ds(me, 1), :].astype(F32), vocab))
    place = place - first
    slot = jnp.where((place >= 0) & (place < cap), owner * cap + place, -1.0)

    def finish(k, carry):
        pair(k, lax.rem(me - k + n, n)).wait_recv()
        pair(k, me).wait_send()
        return carry

    lax.fori_loop(1, n, finish, 0)
    acc_ref[...] = jnp.zeros_like(acc_ref)

    def unpack(group, carry):
        hot = (slot - (group * (GROUP * cap)).astype(F32) == iota((tokens, GROUP * cap), 1)).astype(BF16)
        acc_ref[...] += jnp.dot(hot, rows_ref[pl.ds(group * GROUP, GROUP)].reshape(GROUP * cap, -1),
                                preferred_element_type=F32)
        return carry

    lax.fori_loop(0, n // GROUP, unpack, 0)
    out_ref[...] = acc_ref[...].astype(BF16)


def block_kernel(n, side, do_rows, *refs):
    refs = list(refs)
    take = lambda count: [refs.pop(0) for _ in range(count)]
    if do_rows:
        ids_in, table_in = take(2)
    else:
        (x_in_ref,) = take(1)
    gain_in, w1_in, w2_in, out_ref = take(4)
    if do_rows:
        over_ref, worst_ref = take(2)
    gain_ref, x_ref, acc_ref, w_all, w1_ref, w2_ref, n_ref, send_sem, w_sem, sib_sem, in_sem = take(11)
    if do_rows:
        (ids_ref, table_ref, key_ref, local_ref, owner_ref, hot_ref, pack_ref, mid_ref, turn_ref, last_ref, rows_ref,
         mid_sem, rows_sem) = take(13)
        vocab, tokens = table_ref.shape[0], key_ref.shape[1]

    me = lax.axis_index("tp")
    y, x, core = me // (2 * side), (me // 2) % side, me % 2

    def device(dy, dx, dc=0):
        return (lax.rem(y + dy + side, side) * side + lax.rem(x + dx + side, side)) * 2 + lax.rem(core + dc, 2)

    sent = []

    def send(src, dst, recv_sem, target):
        copy = remote(src, dst, send_sem.at[len(sent)], recv_sem, target)
        copy.start()
        sent.append(copy)

    def wait(ref, recv_sem):
        remote(ref, ref, send_sem.at[0], recv_sem, me).wait_recv()

    greet_all(n, me)
    inputs = [pltpu.make_async_copy(part_in, w_all.at[y, x, core, :, part], in_sem.at[part])
              for part, part_in in enumerate((w1_in, w2_in))]
    inputs += [pltpu.make_async_copy(gain_in, gain_ref, in_sem.at[2])]
    if do_rows:
        inputs += [pltpu.make_async_copy(ids_in, ids_ref, in_sem.at[3]),
                   pltpu.make_async_copy(table_in, table_ref, in_sem.at[4])]
        inputs[3].start()
    for copy in inputs[:3] + inputs[4:]:
        copy.start()

    def piece(half, a, b, owner_core):
        dx, dy = (a, b) if half == 0 else (b, a)
        return w_all.at[lax.rem(y - dy + side, side), lax.rem(x - dx + side, side), owner_core, half]

    def along(half, first, step):
        return device(0, step) if (half == 0) == first else device(step, 0)

    def spot(a, b):
        return a * side + b

    def second_axis(half, a):
        here = piece(half, a, 0, core)
        send(here, here, w_sem.at[half, 0, spot(a, 1)], along(half, False, 1))
        send(here, here, w_sem.at[half, 0, spot(a, 3)], along(half, False, -1))

    def to_sibling(half, a, b):
        here = piece(half, a, b, core)
        send(here, here, sib_sem.at[half, spot(a, b)], device(0, 0, 1))

    def got(half, a, b):
        here = piece(half, a, b, core)
        if b == 2 or (a, b) == (2, 0):
            for part in range(2):
                wait(here.at[part], w_sem.at[half, part, spot(a, b)])
        else:
            wait(here, w_sem.at[half, 0, spot(a, b)])
        if (a, b) == (1, 0):
            send(here.at[0], here.at[0], w_sem.at[half, 0, spot(2, 0)], along(half, True, 1))
        if (a, b) == (3, 0):
            send(here.at[1], here.at[1], w_sem.at[half, 1, spot(2, 0)], along(half, True, -1))
        if b == 1:
            send(here.at[0], here.at[0], w_sem.at[half, 0, spot(a, 2)], along(half, False, 1))
        if b == 3:
            send(here.at[1], here.at[1], w_sem.at[half, 1, spot(a, 2)], along(half, False, -1))
        to_sibling(half, a, b)

    def got_all(*spots):
        for a, b in spots:
            for half in range(2):
                got(half, a, b)

    def spread(*firsts):
        for a in firsts:
            for half in range(2):
                second_axis(half, a)

    def sibling(b):
        for half in range(2):
            for a in range(side):
                wait(piece(half, a, b, 1 - core), sib_sem.at[half, spot(a, b)])

    def line_device(half, line, i):
        in_x, in_y = (i * side + line) * 2, (line * side + i) * 2 + 1
        return in_x if isinstance(half, int) and half == 0 else in_y if isinstance(half, int) else jnp.where(half == 0, in_x, in_y)

    if do_rows:
        inputs[3].wait()
        ids = by_destination(ids_ref, n)
        local = ids - (me * vocab).astype(F32)
        owned = ones((local >= 0) & (local < vocab))
        dy, dx, dc = coords(iota((n, n), 0), side)
        ey, ex, ec = coords(iota((n, n), 1), side)
        same_line = ones(dc == ec) * jnp.where(dc == 0, ones(dx == ex), ones(dy == ey))
        earlier = same_line * jnp.where(dc == 0, ones(ey < dy), ones(ex < dx))
        in_line = jnp.dot(earlier.astype(BF16), owned.astype(BF16), preferred_element_type=F32)
        rank = count_before(owned) + jnp.sum(in_line, axis=1, keepdims=True)
        key_ref[...] = jnp.where(owned > 0, rank, -1.0)
        local_ref[...] = local + 1.0
        owner_ref[...] = owner_of(ids, vocab)

    inputs[0].wait()
    inputs[1].wait()
    pl.semaphore_wait(pltpu.get_barrier_semaphore(), n - 1)
    for half in range(2):
        here = piece(half, 0, 0, core)
        send(here, here, w_sem.at[half, 0, spot(1, 0)], along(half, True, 1))
        send(here, here, w_sem.at[half, 0, spot(3, 0)], along(half, True, -1))
    spread(0)
    for half in range(2):
        to_sibling(half, 0, 0)
    inputs[2].wait()

    if do_rows:
        first_axis = jnp.where(core == 0, x, y)
        last_axis = jnp.where(core == 0, y, x)
        turn_cap, last_cap = mid_ref.shape[1], rows_ref.shape[1]

        def pack(half, line):
            row = jnp.zeros((turn_cap, 1), F32)
            for i in range(side):
                dest = line_device(half, line, i)
                key, val = key_ref[pl.ds(dest, 1), :], local_ref[pl.ds(dest, 1), :]
                row += jnp.sum(jnp.where(key == iota((turn_cap, tokens), 0), val, 0.0), axis=1, keepdims=True)
            hot_ref[...] = (row - 1.0 == iota((turn_cap, vocab), 1)).astype(BF16)
            return jnp.dot(hot_ref[...], table_ref[...], preferred_element_type=F32).astype(BF16)

        inputs[4].wait()
        todo = []
        for step in (1, 3, 2):
            for half in range(2):
                at = len(todo)
                here = x if half == 0 else y
                pack_ref[at] = pack(half, lax.rem(here + step, side))
                target = (y * side + lax.rem(x + step, side)) * 2 if half == 0 else (lax.rem(y + step, side) * side + x) * 2 + 1
                todo.append((at, here * 2 + core, mid_sem.at[step * 2 + core], target))
                if at > 0:
                    at, j, sem, target = todo[at - 1]
                    send(pack_ref.at[at], mid_ref.at[j], sem, target)
            if step == 3:
                got_all((1, 0), (3, 0))
        at = len(todo)
        pack_ref[at] = pack(1 - core, last_axis)
        send(pack_ref.at[at - 1], mid_ref.at[todo[-1][1]], todo[-1][2], todo[-1][3])
        mid_ref[first_axis * 2 + core] = pack(core, first_axis)
        send(pack_ref.at[at], mid_ref.at[last_axis * 2 + core], mid_sem.at[0], device(0, 0, 1))
        spread(1)

        j = lax.broadcasted_iota(jnp.int32, (2 * side, 1), 0)
        source = jnp.where(core == 0, y * (2 * side) + j, (j >> 1) * (2 * side) + x * 2 + (j & 1)).astype(F32)
        for i in range(side):
            mine = owner_ref[pl.ds(line_device(core, first_axis, i), 1), :]
            turn_ref[i * 2 * side:(i + 1) * 2 * side, :] = ones(mine == source)
        from_source = turn_ref[...]
        in_block = count_before(from_source)
        r, c = iota((n, n), 0), iota((n, n), 1)
        (ri, _, _), (ci, _, _) = coords(r, side), coords(c, side)
        earlier = (r - ri * (2 * side) == c - ci * (2 * side)) & (ci < ri)
        in_line = jnp.dot(ones(earlier).astype(BF16), from_source.astype(BF16), preferred_element_type=F32)
        slot = in_block + jnp.sum(in_line, axis=1, keepdims=True) + 1.0
        for i in range(side):
            part = slice(i * 2 * side, (i + 1) * 2 * side)
            mask = from_source[part]
            at = jnp.sum(mask * (slot[part] + j.astype(F32) * turn_cap), axis=0, keepdims=True)
            rank = jnp.sum(in_block[part], axis=0, keepdims=True)
            key_ref[i:i + 1, :] = jnp.where(at > 0, rank, -1.0)
            local_ref[i:i + 1, :] = at

        own_y, own_x, _ = coords(owner_ref[pl.ds(me, 1), :], side)
        via, place = place_among(jnp.where(core == 0, own_y, own_x))
        slot = via * last_cap + place

        def count(owner, counts):
            here = jnp.sum(ones(owner_ref[...] == owner.astype(F32)), axis=1, keepdims=True)
            return jnp.where(iota(counts.shape, 1) == owner.astype(F32), here, counts)

        counts = lax.fori_loop(0, n, count, jnp.zeros((n, 128), F32))
        exact = functools.partial(jnp.dot, precision=lax.Precision.HIGHEST, preferred_element_type=F32)
        bundles = exact(same_line, counts)
        oy, ox, _ = coords(iota((128, 128), 0), side)
        g = iota((128, 128), 1)
        blocks = exact(counts, ones((oy == g) | ((oy < side) & (ox == g - side))))
        lane = iota((n, 128), 1)
        dest_core = coords(iota((n, 128), 0), side)[2]
        counted = jnp.where(dest_core == 0, ones(lane < side), ones((lane >= side) & (lane < 2 * side)))
        over = ones(bundles > turn_cap) + counted * ones(blocks > last_cap)
        over_ref[0] = jnp.max(over)
        worst_ref[0] = jnp.max(counts)

        wait(mid_ref.at[first_axis * 2 + 1 - core], mid_sem.at[0])
        for step in (1, 3, 2):
            for sc in range(2):
                wait(mid_ref.at[lax.rem(first_axis - step + side, side) * 2 + sc], mid_sem.at[step * 2 + sc])

        def turn(step):
            i = lax.rem(last_axis + step, side)
            key, val = key_ref[pl.ds(i, 1), :], local_ref[pl.ds(i, 1), :]
            row = jnp.sum(jnp.where(key == iota((last_cap, tokens), 0), val, 0.0), axis=1, keepdims=True) - 1.0
            hot = (row == iota((last_cap, 2 * side * turn_cap), 1)).astype(BF16)
            return jnp.dot(hot, mid_ref[...].reshape(2 * side * turn_cap, -1), preferred_element_type=F32).astype(BF16)

        def send_turn(step):
            send(last_ref.at[step], rows_ref.at[last_axis], rows_sem.at[step],
                 jnp.where(core == 0, device(step, 0), device(0, step)))

        last_ref[1] = turn(1)
        last_ref[3] = turn(3)
        send_turn(1)
        last_ref[2] = turn(2)
        send_turn(3)
        rows_ref[last_axis] = turn(0)
        send_turn(2)
        got_all((0, 1), (0, 3))
        spread(3)
        got_all((2, 0))
        spread(2)
        got_all((1, 1), (1, 3))

        for step in (1, 3, 2):
            wait(rows_ref.at[lax.rem(last_axis - step + side, side)], rows_sem.at[step])
        hot = (slot == iota((tokens, side * last_cap), 1)).astype(BF16)
        x_ref[...] = jnp.dot(hot, rows_ref[...].reshape(side * last_cap, -1), preferred_element_type=F32).astype(BF16)
    else:
        x_ref[...] = x_in_ref[...]
        got_all((1, 0), (3, 0))
        spread(1, 3)
        got_all((2, 0))
        spread(2)
        got_all((0, 1), (0, 3), (1, 1), (1, 3), (3, 1), (3, 3), (2, 1), (2, 3), (0, 2), (1, 2), (3, 2), (2, 2))

    gain = jnp.concatenate([gain_ref[i:i + 1, :] for i in range(gain_ref.shape[0])], axis=1).astype(F32)
    rows = x_ref[...].astype(F32)
    inv_rms = lax.rsqrt(jnp.mean(rows * rows, axis=-1, keepdims=True) + RMS_EPS)
    n_ref[...] = (rows * inv_rms * gain).astype(BF16)
    acc_ref[...] = jnp.zeros_like(acc_ref)
    span = w1_ref.shape[0] // 2
    tile = min(256, acc_ref.shape[0])

    def mlp(b, owner_core=None):
        row, col = lax.rem(y - b + side, side), lax.rem(x - b + side, side)
        cores = slice(None) if owner_core is None else pl.ds(owner_core, 1)
        width = 2 * span if owner_core is None else span
        for part, dst in enumerate((w1_ref, w2_ref)):
            dst[:width // 2] = w_all[row, :, cores, 0, part].reshape(width // 2, -1)
            dst[width // 2:width] = w_all[:, col, cores, 1, part].reshape(width // 2, -1)

        def step(t, carry):
            at = pl.ds(pl.multiple_of(t * tile, tile), tile)
            u = lax.dot_general(n_ref[at, :], w1_ref[:width], (((1,), (1,)), ((), ())), preferred_element_type=F32)
            h = gelu(u.astype(BF16).astype(F32)).astype(BF16)
            acc_ref[at, :] += jnp.dot(h, w2_ref[:width], preferred_element_type=F32)
            return carry

        lax.fori_loop(0, acc_ref.shape[0] // tile, step, 0)

    if do_rows:
        sibling(0)
        mlp(0)
        got_all((3, 1), (3, 3), (2, 1), (2, 3))
        sibling(1)
        mlp(1)
        got_all((0, 2), (1, 2))
        sibling(3)
        mlp(3)
        got_all((3, 2), (2, 2))
        mlp(2, core)
        sibling(2)
        mlp(2, 1 - core)
    else:
        for b in range(side):
            sibling(b)

        def every(b, carry):
            mlp(b)
            return carry

        lax.fori_loop(0, side, every, 0)
    out_ref[...] = (x_ref[...].astype(F32) + acc_ref[...]).astype(BF16)
    for copy in sent:
        copy.wait_send()


def params(collective_id):
    return pltpu.CompilerParams(collective_id=collective_id, has_side_effects=True, vmem_limit_bytes=VMEM_LIMIT)


def rows_call(n, tokens, dim, vocab):
    vmem, dma = pltpu.VMEM, pltpu.SemaphoreType.DMA
    spec = pl.BlockSpec(memory_space=pltpu.VMEM)
    return pl.pallas_call(
        functools.partial(rows_kernel, n, CAP),
        out_shape=jax.ShapeDtypeStruct((tokens, dim), BF16),
        in_specs=[pl.BlockSpec(memory_space=pltpu.SMEM), spec, spec],
        out_specs=spec,
        scratch_shapes=[vmem((n, tokens), F32), vmem((n, tokens), F32), vmem((GROUP, CAP, vocab), BF16),
                        vmem((n, CAP, dim), BF16), vmem((n, CAP, dim), BF16), vmem((tokens, dim), F32),
                        dma((n,)), dma((n,))],
        compiler_params=params(0))


def block_call(n, side, do_rows, tokens, dim, vocab, share):
    vmem, dma = pltpu.VMEM, pltpu.SemaphoreType.DMA
    spec, hbm = pl.BlockSpec(memory_space=pltpu.VMEM), pl.BlockSpec(memory_space=pltpu.HBM)
    out_shape = [jax.ShapeDtypeStruct((tokens, dim), BF16)]
    sends = 2 * (4 + 16 + side * side) + (7 + 3 if do_rows else 0)
    scratch = [vmem((dim // 128, 128), BF16), vmem((tokens, dim), BF16), vmem((tokens, dim), F32),
               vmem((side, side, 2, 2, 2, share // 2, dim), BF16), vmem((n * share // side, dim), BF16),
               vmem((n * share // side, dim), BF16), vmem((tokens, dim), BF16),
               dma((sends,)), dma((2, 2, side * side)), dma((2, side * side)), dma((5,))]
    if do_rows:
        out_shape += [jax.ShapeDtypeStruct((1,), F32)] * 2
        scratch += [vmem((n * tokens // 128, 128), jnp.int32), vmem((vocab, dim), BF16)] + [vmem((n, tokens), F32)] * 3 + [
            vmem((TURN_CAP, vocab), BF16), vmem((2 * side - 1, TURN_CAP, dim), BF16), vmem((2 * side, TURN_CAP, dim), BF16),
            vmem((n, tokens), F32), vmem((side, LAST_CAP, dim), BF16), vmem((side, LAST_CAP, dim), BF16),
            dma((2 * side,)), dma((side,))]
    return pl.pallas_call(
        functools.partial(block_kernel, n, side, do_rows),
        out_shape=out_shape,
        in_specs=([hbm, hbm] if do_rows else [spec]) + [hbm] * 3,
        out_specs=[spec] + [pl.BlockSpec(memory_space=pltpu.SMEM)] * (len(out_shape) - 1),
        scratch_shapes=scratch,
        compiler_params=params(1 + do_rows))


def solution(mesh):
    n = mesh.shape["tp"]
    side = math.isqrt(n // 2)

    def device_step(token_ids, table_shard, norm_gain, w_in_shard, w_out_shard):
        vocab, dim = table_shard.shape
        share = w_out_shard.shape[0]
        tokens = token_ids.shape[0] // n
        ids = token_ids.reshape(n, tokens)
        block = (norm_gain.reshape(dim // 128, 128), w_in_shard.T.reshape(2, share // 2, dim),
                 w_out_shard.reshape(2, share // 2, dim))
        out, over, worst = block_call(n, side, True, tokens, dim, vocab, share)(
            token_ids.reshape(n * tokens // 128, 128), table_shard, *block)

        def in_rounds():
            rounds = lax.div(worst[0].astype(jnp.int32) + CAP - 1, CAP)

            def one(carry):
                r, rows = carry
                return r + 1, rows + rows_call(n, tokens, dim, vocab)(r.reshape(1), ids, table_shard)

            _, rows = lax.while_loop(lambda carry: carry[0] < rounds, one,
                                     (jnp.int32(0), jnp.zeros((tokens, dim), BF16)))
            return block_call(n, side, False, tokens, dim, vocab, share)(rows, *block)[0]

        return lax.cond(over[0] > 0, in_rounds, lambda: out)

    return jax.shard_map(
        device_step,
        mesh=mesh,
        in_specs=(P("dp"), P("tp", None), P(), P(None, "tp"), P("tp", None)),
        out_specs=P(("dp", "tp"), None),
        check_vma=False,
    )
```

```python
import functools
import math

import jax
import jax.numpy as jnp
from jax import lax
from jax.experimental import pallas as pl
from jax.experimental.pallas import tpu as pltpu
from jax.sharding import PartitionSpec as P

RMS_EPS = 1e-6
MESH = pl.DeviceIdType.MESH
TURN_CAP, LAST_CAP = 224, 272
CAP, GROUP = 64, 8
VMEM_LIMIT = 44 * 2**20
DIRECT = (3,)
EARLY = 2
GELU_SCALE = math.sqrt(2.0 / math.pi)
F32, BF16 = jnp.float32, jnp.bfloat16


def iota(shape, dim):
    return lax.broadcasted_iota(jnp.int32, shape, dim).astype(F32)


def ones(mask):
    return jnp.where(mask, 1.0, 0.0)


def count_before(mask):
    tokens = mask.shape[1]
    before = ones(iota((tokens, tokens), 0) < iota((tokens, tokens), 1)).astype(BF16)
    return jnp.dot(mask.astype(BF16), before, preferred_element_type=F32)


def as_column(row):
    tokens = row.shape[1]
    return jnp.sum(jnp.where(iota((tokens, tokens), 0) == iota((tokens, tokens), 1), row, 0.0), axis=1, keepdims=True)


def place_among(kind):
    column = as_column(kind)
    tokens = kind.shape[1]
    same = (column == kind) & (iota((tokens, tokens), 1) < iota((tokens, tokens), 0))
    return column, jnp.sum(ones(same), axis=1, keepdims=True)


def coords(device, side):
    y = jnp.floor((device + 0.5) * (0.5 / side))
    x = jnp.floor((device - y * (2 * side) + 0.5) * 0.5)
    return y, x, device - y * (2 * side) - x * 2


def owner_of(ids, vocab):
    return jnp.floor((ids + 0.5) * (1.0 / vocab))


def gelu(z):
    return (0.5 * z) * (1.0 + jnp.tanh(z * (GELU_SCALE + GELU_SCALE * 0.044715 * (z * z))))


def by_destination(ids_ref, n):
    each = ids_ref.shape[0] // n
    return jnp.concatenate([ids_ref[pl.ds(j, n, stride=each), :] for j in range(each)], axis=1).astype(F32)


def greet_all(n, me):
    def greet(k, carry):
        pl.semaphore_signal(pltpu.get_barrier_semaphore(), inc=1, device_id={"tp": lax.rem(me + k, n)},
                            device_id_type=MESH)
        return carry

    lax.fori_loop(1, n, greet, 0)


def remote(src, dst, send_sem, recv_sem, target):
    return pltpu.make_async_remote_copy(src_ref=src, dst_ref=dst, send_sem=send_sem, recv_sem=recv_sem,
                                        device_id={"tp": target}, device_id_type=MESH)


def rows_kernel(n, cap, round_ref, ids_ref, table_ref, out_ref, key_ref, local_ref, hot_ref, pack_ref, rows_ref, acc_ref,
                send_sem, rows_sem):
    vocab, tokens = table_ref.shape[0], ids_ref.shape[1]
    me = lax.axis_index("tp")
    greet_all(n, me)
    local = ids_ref[...].astype(F32) - (me * vocab).astype(F32)
    owned = (local >= 0) & (local < vocab)
    first = (round_ref[0] * cap).astype(F32)
    key_ref[...] = jnp.where(owned, count_before(ones(owned)) - first, -1.0)
    local_ref[...] = local + 1.0
    pl.semaphore_wait(pltpu.get_barrier_semaphore(), n - 1)

    def pack(group, carry):
        def fill(j, carry):
            dest = lax.rem(me + group * GROUP + j, n)
            key, val = key_ref[pl.ds(dest, 1), :], local_ref[pl.ds(dest, 1), :]
            row = jnp.sum(jnp.where(key == iota((cap, tokens), 0), val, 0.0), axis=1, keepdims=True) - 1.0
            hot_ref[j] = (row == iota((cap, vocab), 1)).astype(BF16)
            return carry

        lax.fori_loop(0, GROUP, fill, 0)
        rows = jnp.dot(hot_ref[...].reshape(GROUP * cap, vocab), table_ref[...], preferred_element_type=F32)
        pack_ref[pl.ds(group * GROUP, GROUP)] = rows.astype(BF16).reshape(GROUP, cap, -1)
        return carry

    lax.fori_loop(0, n // GROUP, pack, 0)

    def pair(k, source):
        return remote(pack_ref.at[k], rows_ref.at[source], send_sem.at[k], rows_sem.at[k], lax.rem(me + k, n))

    def start(k, carry):
        pair(k, me).start()
        return carry

    lax.fori_loop(1, n, start, 0)
    rows_ref[me] = pack_ref[0]
    owner, place = place_among(owner_of(ids_ref[pl.ds(me, 1), :].astype(F32), vocab))
    place = place - first
    slot = jnp.where((place >= 0) & (place < cap), owner * cap + place, -1.0)

    def finish(k, carry):
        pair(k, lax.rem(me - k + n, n)).wait_recv()
        pair(k, me).wait_send()
        return carry

    lax.fori_loop(1, n, finish, 0)
    acc_ref[...] = jnp.zeros_like(acc_ref)

    def unpack(group, carry):
        hot = (slot - (group * (GROUP * cap)).astype(F32) == iota((tokens, GROUP * cap), 1)).astype(BF16)
        acc_ref[...] += jnp.dot(hot, rows_ref[pl.ds(group * GROUP, GROUP)].reshape(GROUP * cap, -1),
                                preferred_element_type=F32)
        return carry

    lax.fori_loop(0, n // GROUP, unpack, 0)
    out_ref[...] = acc_ref[...].astype(BF16)


def block_kernel(n, side, do_rows, *refs):
    refs = list(refs)
    take = lambda count: [refs.pop(0) for _ in range(count)]
    if do_rows:
        ids_in, table_in = take(2)
    else:
        (x_in_ref,) = take(1)
    gain_in, w1_in, w2_in, out_ref = take(4)
    if do_rows:
        over_ref, worst_ref = take(2)
    gain_ref, x_ref, acc_ref, w_all, w1_ref, w2_ref, n_ref, send_sem, w_sem, sib_sem, in_sem = take(11)
    if do_rows:
        (ids_ref, table_ref, key_ref, local_ref, owner_ref, hot_ref, pack_ref, mid_ref, turn_ref, last_ref, rows_ref,
         mid_sem, rows_sem) = take(13)
        vocab, tokens = table_ref.shape[0], key_ref.shape[1]

    me = lax.axis_index("tp")
    y, x, core = me // (2 * side), (me // 2) % side, me % 2

    def device(dy, dx, dc=0):
        return (lax.rem(y + dy + side, side) * side + lax.rem(x + dx + side, side)) * 2 + lax.rem(core + dc, 2)

    sent = []

    def send(src, dst, recv_sem, target):
        copy = remote(src, dst, send_sem.at[len(sent)], recv_sem, target)
        copy.start()
        sent.append(copy)

    def wait(ref, recv_sem):
        remote(ref, ref, send_sem.at[0], recv_sem, me).wait_recv()

    partners = [device(0, 0, 1)]
    for step in (2, 1, 3):
        for other in range(2):
            partners += [device(0, step, other), device(step, 0, other)]
    for partner in partners:
        pl.semaphore_signal(pltpu.get_barrier_semaphore(), inc=1, device_id={"tp": partner}, device_id_type=MESH)
    inputs = [pltpu.make_async_copy(part_in, w_all.at[y, x, core, :, part], in_sem.at[part])
              for part, part_in in enumerate((w1_in, w2_in))]
    inputs += [pltpu.make_async_copy(gain_in, gain_ref, in_sem.at[2])]
    if do_rows:
        inputs += [pltpu.make_async_copy(ids_in, ids_ref, in_sem.at[3]),
                   pltpu.make_async_copy(table_in, table_ref, in_sem.at[4])]
        inputs[3].start()
    for copy in inputs[:3] + inputs[4:]:
        copy.start()

    def piece(half, a, b, owner_core):
        dx, dy = (a, b) if half == 0 else (b, a)
        return w_all.at[lax.rem(y - dy + side, side), lax.rem(x - dx + side, side), owner_core, half]

    def along(half, first, step):
        return device(0, step) if (half == 0) == first else device(step, 0)

    def spot(a, b):
        return a * side + b

    def second_axis(half, a):
        here = piece(half, a, 0, core)
        if a in DIRECT:
            send(here, here, w_sem.at[half, 0, spot(a, 2)], along(half, False, 2))
        send(here, here, w_sem.at[half, 0, spot(a, 1)], along(half, False, 1))
        send(here, here, w_sem.at[half, 0, spot(a, 3)], along(half, False, -1))

    def to_sibling(half, a, b):
        here = piece(half, a, b, core)
        send(here, here, sib_sem.at[half, spot(a, b)], device(0, 0, 1))

    def got(half, a, b):
        here = piece(half, a, b, core)
        if (b == 2 and a not in DIRECT) or (a, b) == (2, 0):
            for part in range(2):
                wait(here.at[part], w_sem.at[half, part, spot(a, b)])
        else:
            wait(here, w_sem.at[half, 0, spot(a, b)])
        if (a, b) == (1, 0):
            send(here.at[0], here.at[0], w_sem.at[half, 0, spot(2, 0)], along(half, True, 1))
        if (a, b) == (3, 0):
            send(here.at[1], here.at[1], w_sem.at[half, 1, spot(2, 0)], along(half, True, -1))
        if b == 1 and a not in DIRECT:
            send(here.at[0], here.at[0], w_sem.at[half, 0, spot(a, 2)], along(half, False, 1))
        if b == 3 and a not in DIRECT:
            send(here.at[1], here.at[1], w_sem.at[half, 1, spot(a, 2)], along(half, False, -1))
        to_sibling(half, a, b)

    def parse(spots):
        return [(int(a), int(b)) for a, b in spots.split()]

    def got_all(spots):
        for a, b in parse(spots):
            for half in range(2):
                got(half, a, b)

    def from_sibling(spots):
        for a, b in parse(spots):
            for half in range(2):
                wait(piece(half, a, b, 1 - core), sib_sem.at[half, spot(a, b)])

    def spread(*firsts):
        for a in firsts:
            for half in range(2):
                second_axis(half, a)

    def line_device(half, line, i):
        in_x, in_y = (i * side + line) * 2, (line * side + i) * 2 + 1
        return in_x if isinstance(half, int) and half == 0 else in_y if isinstance(half, int) else jnp.where(half == 0, in_x, in_y)

    if do_rows:
        inputs[3].wait()
        ids = by_destination(ids_ref, n)
        local = ids - (me * vocab).astype(F32)
        owned = ones((local >= 0) & (local < vocab))
        dy, dx, dc = coords(iota((n, n), 0), side)
        ey, ex, ec = coords(iota((n, n), 1), side)
        same_line = ones(dc == ec) * jnp.where(dc == 0, ones(dx == ex), ones(dy == ey))
        earlier = same_line * jnp.where(dc == 0, ones(ey < dy), ones(ex < dx))
        in_line = jnp.dot(earlier.astype(BF16), owned.astype(BF16), preferred_element_type=F32)
        rank = count_before(owned) + jnp.sum(in_line, axis=1, keepdims=True)
        key_ref[...] = jnp.where(owned > 0, rank, -1.0)
        local_ref[...] = local + 1.0
        owner_ref[...] = owner_of(ids, vocab)

    def enter():
        inputs[0].wait()
        inputs[1].wait()
        pl.semaphore_wait(pltpu.get_barrier_semaphore(), len(partners))
        for half in range(2):
            here = piece(half, 0, 0, core)
            send(here, here, w_sem.at[half, 0, spot(1, 0)], along(half, True, 1))
            send(here, here, w_sem.at[half, 0, spot(3, 0)], along(half, True, -1))

    def own():
        spread(0)
        for half in range(2):
            to_sibling(half, 0, 0)
        inputs[2].wait()

    if do_rows:
        first_axis = jnp.where(core == 0, x, y)
        last_axis = jnp.where(core == 0, y, x)
        turn_cap, last_cap = mid_ref.shape[1], rows_ref.shape[1]

        def pack(half, line):
            row = jnp.zeros((turn_cap, 1), F32)
            for i in range(side):
                dest = line_device(half, line, i)
                key, val = key_ref[pl.ds(dest, 1), :], local_ref[pl.ds(dest, 1), :]
                row += jnp.sum(jnp.where(key == iota((turn_cap, tokens), 0), val, 0.0), axis=1, keepdims=True)
            hot_ref[...] = (row - 1.0 == iota((turn_cap, vocab), 1)).astype(BF16)
            return jnp.dot(hot_ref[...], table_ref[...], preferred_element_type=F32).astype(BF16)

        inputs[4].wait()
        bundles = []
        for step in (2, 1, 3):
            for half in range(2):
                at, here = len(bundles), (x, y)[half]
                pack_ref[at] = pack(half, lax.rem(here + step, side))
                target = ((y * side + lax.rem(x + step, side)) * 2, (lax.rem(y + step, side) * side + x) * 2 + 1)[half]
                bundles.append((pack_ref.at[at], mid_ref.at[here * 2 + core], mid_sem.at[step * 2 + core], target))
                if at == EARLY:
                    enter()
                    for bundle in bundles[:-1]:
                        send(*bundle)
                elif at > EARLY:
                    send(*bundles[-2])
        pack_ref[len(bundles)] = pack(1 - core, last_axis)
        send(*bundles[-1])
        own()
        mid_ref[first_axis * 2 + core] = pack(core, first_axis)
        send(pack_ref.at[len(bundles)], mid_ref.at[last_axis * 2 + core], mid_sem.at[0], device(0, 0, 1))

        j = lax.broadcasted_iota(jnp.int32, (2 * side, 1), 0)
        source = jnp.where(core == 0, y * (2 * side) + j, (j >> 1) * (2 * side) + x * 2 + (j & 1)).astype(F32)
        for i in range(side):
            mine = owner_ref[pl.ds(line_device(core, first_axis, i), 1), :]
            turn_ref[i * 2 * side:(i + 1) * 2 * side, :] = ones(mine == source)
        from_source = turn_ref[...]
        in_block = count_before(from_source)
        r, c = iota((n, n), 0), iota((n, n), 1)
        (ri, _, _), (ci, _, _) = coords(r, side), coords(c, side)
        earlier = (r - ri * (2 * side) == c - ci * (2 * side)) & (ci < ri)
        in_line = jnp.dot(ones(earlier).astype(BF16), from_source.astype(BF16), preferred_element_type=F32)
        slot = in_block + jnp.sum(in_line, axis=1, keepdims=True) + 1.0
        for i in range(side):
            part = slice(i * 2 * side, (i + 1) * 2 * side)
            mask = from_source[part]
            at = jnp.sum(mask * (slot[part] + j.astype(F32) * turn_cap), axis=0, keepdims=True)
            rank = jnp.sum(in_block[part], axis=0, keepdims=True)
            key_ref[i:i + 1, :] = jnp.where(at > 0, rank, -1.0)
            local_ref[i:i + 1, :] = at

        own_y, own_x, _ = coords(owner_ref[pl.ds(me, 1), :], side)
        via, place = place_among(jnp.where(core == 0, own_y, own_x))
        slot = via * last_cap + place

        def count(owner, counts):
            here = jnp.sum(ones(owner_ref[...] == owner.astype(F32)), axis=1, keepdims=True)
            return jnp.where(iota(counts.shape, 1) == owner.astype(F32), here, counts)

        counts = lax.fori_loop(0, n, count, jnp.zeros((n, 128), F32))
        exact = functools.partial(jnp.dot, precision=lax.Precision.HIGHEST, preferred_element_type=F32)
        in_bundle = exact(same_line, counts)
        oy, ox, _ = coords(iota((128, 128), 0), side)
        g = iota((128, 128), 1)
        blocks = exact(counts, ones((oy == g) | ((oy < side) & (ox == g - side))))
        lane = iota((n, 128), 1)
        dest_core = coords(iota((n, 128), 0), side)[2]
        counted = jnp.where(dest_core == 0, ones(lane < side), ones((lane >= side) & (lane < 2 * side)))
        over = ones(in_bundle > turn_cap) + counted * ones(blocks > last_cap)
        over_ref[0] = jnp.max(over)
        worst_ref[0] = jnp.max(counts)

        got_all("10 30")
        spread(1)
        wait(mid_ref.at[first_axis * 2 + 1 - core], mid_sem.at[0])
        for step in (1, 3, 2):
            for sc in range(2):
                wait(mid_ref.at[lax.rem(first_axis - step + side, side) * 2 + sc], mid_sem.at[step * 2 + sc])

        def turn(step):
            i = lax.rem(last_axis + step, side)
            key, val = key_ref[pl.ds(i, 1), :], local_ref[pl.ds(i, 1), :]
            row = jnp.sum(jnp.where(key == iota((last_cap, tokens), 0), val, 0.0), axis=1, keepdims=True) - 1.0
            hot = (row == iota((last_cap, 2 * side * turn_cap), 1)).astype(BF16)
            return jnp.dot(hot, mid_ref[...].reshape(2 * side * turn_cap, -1), preferred_element_type=F32).astype(BF16)

        def send_turn(step):
            send(last_ref.at[step], rows_ref.at[last_axis], rows_sem.at[step],
                 jnp.where(core == 0, device(step, 0), device(0, step)))

        last_ref[2] = turn(2)
        last_ref[1] = turn(1)
        send_turn(2)
        last_ref[3] = turn(3)
        send_turn(1)
        rows_ref[last_axis] = turn(0)
        send_turn(3)
        got_all("01 03 20")
        spread(2)
        got_all("11 13")
        spread(3)

        for step in (1, 3, 2):
            wait(rows_ref.at[lax.rem(last_axis - step + side, side)], rows_sem.at[step])
        hot = (slot == iota((tokens, side * last_cap), 1)).astype(BF16)
        x_ref[...] = jnp.dot(hot, rows_ref[...].reshape(side * last_cap, -1), preferred_element_type=F32).astype(BF16)
    else:
        x_ref[...] = x_in_ref[...]
        enter()
        own()
        got_all("10 30")
        spread(1, 3)
        got_all("20")
        spread(2)
        for spots in ("01 03 11 13", "31 33 21 23", "02 12 32 22"):
            got_all(spots)

    gain = jnp.concatenate([gain_ref[i:i + 1, :] for i in range(gain_ref.shape[0])], axis=1).astype(F32)
    rows = x_ref[...].astype(F32)
    inv_rms = lax.rsqrt(jnp.mean(rows * rows, axis=-1, keepdims=True) + RMS_EPS)
    n_ref[...] = (rows * inv_rms * gain).astype(BF16)
    acc_ref[...] = jnp.zeros_like(acc_ref)
    span = 2 * w_all.shape[5]

    def mlp(spots, owner_core=None):
        spots = parse(spots) if isinstance(spots, str) else spots
        cores = slice(None) if owner_core is None else pl.ds(owner_core, 1)
        rows = span if owner_core is None else span // 2
        width = 2 * len(spots) * rows
        for part, dst in enumerate((w1_ref, w2_ref)):
            at = 0
            for a, b in spots:
                for dx, dy, half in ((a, b, 0), (b, a, 1)):
                    row, col = lax.rem(y - dy + side, side), lax.rem(x - dx + side, side)
                    dst[at:at + rows] = w_all[row, col, cores, half, part].reshape(rows, -1)
                    at += rows

        u = lax.dot_general(n_ref[...], w1_ref[:width], (((1,), (1,)), ((), ())), preferred_element_type=F32)
        h = gelu(u.astype(BF16).astype(F32)).astype(BF16)
        acc_ref[...] += jnp.dot(h, w2_ref[:width], preferred_element_type=F32)

    if do_rows:
        from_sibling("00 10 20 30")
        mlp("00 10 20 30")
        got_all("02 21 23")
        from_sibling("01 03 11 13")
        mlp("01 03 11 13")
        got_all("12")
        mlp("02 12 21 23", core)
        from_sibling("02 21 23 12")
        mlp("02 12 21 23", 1 - core)
        got_all("31 33 32 22")
        mlp("31 33 32 22", core)
        from_sibling("31 33 32 22")
        mlp("31 33 32 22", 1 - core)
    else:
        def every(a, carry):
            mlp([(a, b) for b in range(side)])
            return carry

        for spots in ("00 01 02 03", "10 11 12 13", "20 21 22 23", "30 31 32 33"):
            from_sibling(spots)
        lax.fori_loop(0, side, every, 0)
    out_ref[...] = (x_ref[...].astype(F32) + acc_ref[...]).astype(BF16)
    for copy in sent:
        copy.wait_send()


def params(collective_id):
    return pltpu.CompilerParams(collective_id=collective_id, has_side_effects=True, vmem_limit_bytes=VMEM_LIMIT)


def rows_call(n, tokens, dim, vocab):
    vmem, dma = pltpu.VMEM, pltpu.SemaphoreType.DMA
    spec = pl.BlockSpec(memory_space=pltpu.VMEM)
    return pl.pallas_call(
        functools.partial(rows_kernel, n, CAP),
        out_shape=jax.ShapeDtypeStruct((tokens, dim), BF16),
        in_specs=[pl.BlockSpec(memory_space=pltpu.SMEM), spec, spec],
        out_specs=spec,
        scratch_shapes=[vmem((n, tokens), F32), vmem((n, tokens), F32), vmem((GROUP, CAP, vocab), BF16),
                        vmem((n, CAP, dim), BF16), vmem((n, CAP, dim), BF16), vmem((tokens, dim), F32),
                        dma((n,)), dma((n,))],
        compiler_params=params(0))


def block_call(n, side, do_rows, tokens, dim, vocab, share):
    vmem, dma = pltpu.VMEM, pltpu.SemaphoreType.DMA
    spec, hbm = pl.BlockSpec(memory_space=pltpu.VMEM), pl.BlockSpec(memory_space=pltpu.HBM)
    out_shape = [jax.ShapeDtypeStruct((tokens, dim), BF16)]
    sends = 2 * (4 + 16 - len(DIRECT) + side * side) + (7 + 3 if do_rows else 0)
    scratch = [vmem((dim // 128, 128), BF16), vmem((tokens, dim), BF16), vmem((tokens, dim), F32),
               vmem((side, side, 2, 2, 2, share // 2, dim), BF16), vmem((n * share // side, dim), BF16),
               vmem((n * share // side, dim), BF16), vmem((tokens, dim), BF16),
               dma((sends,)), dma((2, 2, side * side)), dma((2, side * side)), dma((5,))]
    if do_rows:
        out_shape += [jax.ShapeDtypeStruct((1,), F32)] * 2
        scratch += [vmem((n * tokens // 128, 128), jnp.int32), vmem((vocab, dim), BF16)] + [vmem((n, tokens), F32)] * 3 + [
            vmem((TURN_CAP, vocab), BF16), vmem((2 * side - 1, TURN_CAP, dim), BF16), vmem((2 * side, TURN_CAP, dim), BF16),
            vmem((n, tokens), F32), vmem((side, LAST_CAP, dim), BF16), vmem((side, LAST_CAP, dim), BF16),
            dma((2 * side,)), dma((side,))]
    return pl.pallas_call(
        functools.partial(block_kernel, n, side, do_rows),
        out_shape=out_shape,
        in_specs=([hbm, hbm] if do_rows else [spec]) + [hbm] * 3,
        out_specs=[spec] + [pl.BlockSpec(memory_space=pltpu.SMEM)] * (len(out_shape) - 1),
        scratch_shapes=scratch,
        compiler_params=params(1 + do_rows))


def solution(mesh):
    n = mesh.shape["tp"]
    side = math.isqrt(n // 2)

    def device_step(token_ids, table_shard, norm_gain, w_in_shard, w_out_shard):
        vocab, dim = table_shard.shape
        share = w_out_shard.shape[0]
        tokens = token_ids.shape[0] // n
        ids = token_ids.reshape(n, tokens)
        block = (norm_gain.reshape(dim // 128, 128), w_in_shard.T.reshape(2, share // 2, dim),
                 w_out_shard.reshape(2, share // 2, dim))
        out, over, worst = block_call(n, side, True, tokens, dim, vocab, share)(
            token_ids.reshape(n * tokens // 128, 128), table_shard, *block)

        def in_rounds():
            rounds = lax.div(worst[0].astype(jnp.int32) + CAP - 1, CAP)

            def one(carry):
                r, rows = carry
                return r + 1, rows + rows_call(n, tokens, dim, vocab)(r.reshape(1), ids, table_shard)

            _, rows = lax.while_loop(lambda carry: carry[0] < rounds, one,
                                     (jnp.int32(0), jnp.zeros((tokens, dim), BF16)))
            return block_call(n, side, False, tokens, dim, vocab, share)(rows, *block)[0]

        return lax.cond(over[0] > 0, in_rounds, lambda: out)

    return jax.shard_map(
        device_step,
        mesh=mesh,
        in_specs=(P("dp"), P("tp", None), P(), P(None, "tp"), P("tp", None)),
        out_specs=P(("dp", "tp"), None),
        check_vma=False,
    )
```

```python
import functools
import math

import jax
import jax.numpy as jnp
from jax import lax
from jax.experimental import pallas as pl
from jax.experimental.pallas import tpu as pltpu
from jax.sharding import PartitionSpec as P

RMS_EPS = 1e-6
MESH = pl.DeviceIdType.MESH
TURN_CAP, LAST_CAP = 224, 272
CAP, GROUP = 64, 8
VMEM_LIMIT = 44 * 2**20
DIRECT = (3,)
GELU_SCALE = math.sqrt(2.0 / math.pi)
F32, BF16 = jnp.float32, jnp.bfloat16


def iota(shape, dim):
    return lax.broadcasted_iota(jnp.int32, shape, dim).astype(F32)


def ones(mask):
    return jnp.where(mask, 1.0, 0.0)


def count_before(mask):
    tokens = mask.shape[1]
    before = ones(iota((tokens, tokens), 0) < iota((tokens, tokens), 1)).astype(BF16)
    return jnp.dot(mask.astype(BF16), before, preferred_element_type=F32)


def as_column(row):
    tokens = row.shape[1]
    return jnp.sum(jnp.where(iota((tokens, tokens), 0) == iota((tokens, tokens), 1), row, 0.0), axis=1, keepdims=True)


def place_among(kind):
    column = as_column(kind)
    tokens = kind.shape[1]
    same = (column == kind) & (iota((tokens, tokens), 1) < iota((tokens, tokens), 0))
    return column, jnp.sum(ones(same), axis=1, keepdims=True)


def coords(device, side):
    y = jnp.floor((device + 0.5) * (0.5 / side))
    x = jnp.floor((device - y * (2 * side) + 0.5) * 0.5)
    return y, x, device - y * (2 * side) - x * 2


def owner_of(ids, vocab):
    return jnp.floor((ids + 0.5) * (1.0 / vocab))


def gelu(z):
    return (0.5 * z) * (1.0 + jnp.tanh(z * (GELU_SCALE + GELU_SCALE * 0.044715 * (z * z))))


def by_destination(ids_ref, n):
    each = ids_ref.shape[0] // n
    return jnp.concatenate([ids_ref[pl.ds(j, n, stride=each), :] for j in range(each)], axis=1).astype(F32)


def greet_all(n, me):
    def greet(k, carry):
        pl.semaphore_signal(pltpu.get_barrier_semaphore(), inc=1, device_id={"tp": lax.rem(me + k, n)},
                            device_id_type=MESH)
        return carry

    lax.fori_loop(1, n, greet, 0)


def remote(src, dst, send_sem, recv_sem, target):
    return pltpu.make_async_remote_copy(src_ref=src, dst_ref=dst, send_sem=send_sem, recv_sem=recv_sem,
                                        device_id={"tp": target}, device_id_type=MESH)


def rows_kernel(n, cap, round_ref, ids_ref, table_ref, out_ref, key_ref, local_ref, hot_ref, pack_ref, rows_ref, acc_ref,
                send_sem, rows_sem):
    vocab, tokens = table_ref.shape[0], ids_ref.shape[1]
    me = lax.axis_index("tp")
    greet_all(n, me)
    local = ids_ref[...].astype(F32) - (me * vocab).astype(F32)
    owned = (local >= 0) & (local < vocab)
    first = (round_ref[0] * cap).astype(F32)
    key_ref[...] = jnp.where(owned, count_before(ones(owned)) - first, -1.0)
    local_ref[...] = local + 1.0
    pl.semaphore_wait(pltpu.get_barrier_semaphore(), n - 1)

    def pack(group, carry):
        def fill(j, carry):
            dest = lax.rem(me + group * GROUP + j, n)
            key, val = key_ref[pl.ds(dest, 1), :], local_ref[pl.ds(dest, 1), :]
            row = jnp.sum(jnp.where(key == iota((cap, tokens), 0), val, 0.0), axis=1, keepdims=True) - 1.0
            hot_ref[j] = (row == iota((cap, vocab), 1)).astype(BF16)
            return carry

        lax.fori_loop(0, GROUP, fill, 0)
        rows = jnp.dot(hot_ref[...].reshape(GROUP * cap, vocab), table_ref[...], preferred_element_type=F32)
        pack_ref[pl.ds(group * GROUP, GROUP)] = rows.astype(BF16).reshape(GROUP, cap, -1)
        return carry

    lax.fori_loop(0, n // GROUP, pack, 0)

    def pair(k, source):
        return remote(pack_ref.at[k], rows_ref.at[source], send_sem.at[k], rows_sem.at[k], lax.rem(me + k, n))

    def start(k, carry):
        pair(k, me).start()
        return carry

    lax.fori_loop(1, n, start, 0)
    rows_ref[me] = pack_ref[0]
    owner, place = place_among(owner_of(ids_ref[pl.ds(me, 1), :].astype(F32), vocab))
    place = place - first
    slot = jnp.where((place >= 0) & (place < cap), owner * cap + place, -1.0)

    def finish(k, carry):
        pair(k, lax.rem(me - k + n, n)).wait_recv()
        pair(k, me).wait_send()
        return carry

    lax.fori_loop(1, n, finish, 0)
    acc_ref[...] = jnp.zeros_like(acc_ref)

    def unpack(group, carry):
        hot = (slot - (group * (GROUP * cap)).astype(F32) == iota((tokens, GROUP * cap), 1)).astype(BF16)
        acc_ref[...] += jnp.dot(hot, rows_ref[pl.ds(group * GROUP, GROUP)].reshape(GROUP * cap, -1),
                                preferred_element_type=F32)
        return carry

    lax.fori_loop(0, n // GROUP, unpack, 0)
    out_ref[...] = acc_ref[...].astype(BF16)


def block_kernel(n, side, do_rows, *refs):
    refs = list(refs)
    take = lambda count: [refs.pop(0) for _ in range(count)]
    if do_rows:
        ids_in, table_in = take(2)
    else:
        (x_in_ref,) = take(1)
    gain_in, w1_in, w2_in, out_ref = take(4)
    if do_rows:
        over_ref, worst_ref = take(2)
    gain_ref, x_ref, acc_ref, w_all, w1_ref, w2_ref, n_ref, send_sem, w_sem, sib_sem, in_sem = take(11)
    if do_rows:
        (ids_ref, table_ref, key_ref, local_ref, owner_ref, hot_ref, pack_ref, mid_ref, turn_ref, last_ref, rows_ref,
         mid_sem, rows_sem) = take(13)
        vocab, tokens = table_ref.shape[0], key_ref.shape[1]

    me = lax.axis_index("tp")
    y, x, core = me // (2 * side), (me // 2) % side, me % 2

    def device(dy, dx, dc=0):
        return (lax.rem(y + dy + side, side) * side + lax.rem(x + dx + side, side)) * 2 + lax.rem(core + dc, 2)

    sent = []

    def send(src, dst, recv_sem, target):
        copy = remote(src, dst, send_sem.at[len(sent)], recv_sem, target)
        copy.start()
        sent.append(copy)

    def wait(ref, recv_sem):
        remote(ref, ref, send_sem.at[0], recv_sem, me).wait_recv()

    partners = [device(0, 0, 1)]
    for step in (2, 1, 3):
        for other in range(2):
            partners += [device(0, step, other), device(step, 0, other)]
    for partner in partners:
        pl.semaphore_signal(pltpu.get_barrier_semaphore(), inc=1, device_id={"tp": partner}, device_id_type=MESH)
    inputs = [pltpu.make_async_copy(part_in, w_all.at[y, x, core, :, part], in_sem.at[part])
              for part, part_in in enumerate((w1_in, w2_in))]
    inputs += [pltpu.make_async_copy(gain_in, gain_ref, in_sem.at[2])]
    if do_rows:
        inputs += [pltpu.make_async_copy(ids_in, ids_ref, in_sem.at[3]),
                   pltpu.make_async_copy(table_in, table_ref, in_sem.at[4])]
        inputs[3].start()
    for copy in inputs[:3] + inputs[4:]:
        copy.start()

    def piece(half, a, b, owner_core):
        dx, dy = (a, b) if half == 0 else (b, a)
        return w_all.at[lax.rem(y - dy + side, side), lax.rem(x - dx + side, side), owner_core, half]

    def along(half, first, step):
        return device(0, step) if (half == 0) == first else device(step, 0)

    def spot(a, b):
        return a * side + b

    def second_axis(half, a):
        here = piece(half, a, 0, core)
        if a in DIRECT:
            send(here, here, w_sem.at[half, 0, spot(a, 2)], along(half, False, 2))
        send(here, here, w_sem.at[half, 0, spot(a, 1)], along(half, False, 1))
        send(here, here, w_sem.at[half, 0, spot(a, 3)], along(half, False, -1))

    def to_sibling(half, a, b):
        here = piece(half, a, b, core)
        send(here, here, sib_sem.at[half, spot(a, b)], device(0, 0, 1))

    def got(half, a, b):
        here = piece(half, a, b, core)
        if (b == 2 and a not in DIRECT) or (a, b) == (2, 0):
            for part in range(2):
                wait(here.at[part], w_sem.at[half, part, spot(a, b)])
        else:
            wait(here, w_sem.at[half, 0, spot(a, b)])
        if (a, b) == (1, 0):
            send(here.at[0], here.at[0], w_sem.at[half, 0, spot(2, 0)], along(half, True, 1))
        if (a, b) == (3, 0):
            send(here.at[1], here.at[1], w_sem.at[half, 1, spot(2, 0)], along(half, True, -1))
        if b == 1 and a not in DIRECT:
            send(here.at[0], here.at[0], w_sem.at[half, 0, spot(a, 2)], along(half, False, 1))
        if b == 3 and a not in DIRECT:
            send(here.at[1], here.at[1], w_sem.at[half, 1, spot(a, 2)], along(half, False, -1))
        to_sibling(half, a, b)

    def parse(spots):
        return [(int(a), int(b)) for a, b in spots.split()]

    def got_all(spots):
        for a, b in parse(spots):
            for half in range(2):
                got(half, a, b)

    def from_sibling(spots):
        for a, b in parse(spots):
            for half in range(2):
                wait(piece(half, a, b, 1 - core), sib_sem.at[half, spot(a, b)])

    def spread(*firsts):
        for a in firsts:
            for half in range(2):
                second_axis(half, a)

    def line_device(half, line, i):
        in_x, in_y = (i * side + line) * 2, (line * side + i) * 2 + 1
        return in_x if isinstance(half, int) and half == 0 else in_y if isinstance(half, int) else jnp.where(half == 0, in_x, in_y)

    if do_rows:
        inputs[3].wait()
        ids = by_destination(ids_ref, n)
        local = ids - (me * vocab).astype(F32)
        owned = ones((local >= 0) & (local < vocab))
        dy, dx, dc = coords(iota((n, n), 0), side)
        ey, ex, ec = coords(iota((n, n), 1), side)
        same_line = ones(dc == ec) * jnp.where(dc == 0, ones(dx == ex), ones(dy == ey))
        earlier = same_line * jnp.where(dc == 0, ones(ey < dy), ones(ex < dx))
        in_line = jnp.dot(earlier.astype(BF16), owned.astype(BF16), preferred_element_type=F32)
        rank = count_before(owned) + jnp.sum(in_line, axis=1, keepdims=True)
        key_ref[...] = jnp.where(owned > 0, rank, -1.0)
        local_ref[...] = local + 1.0
        owner_ref[...] = owner_of(ids, vocab)

    def enter():
        inputs[0].wait()
        inputs[1].wait()
        pl.semaphore_wait(pltpu.get_barrier_semaphore(), len(partners))
        for half in range(2):
            here = piece(half, 0, 0, core)
            send(here, here, w_sem.at[half, 0, spot(1, 0)], along(half, True, 1))
            send(here, here, w_sem.at[half, 0, spot(3, 0)], along(half, True, -1))

    def own():
        spread(0)
        for half in range(2):
            to_sibling(half, 0, 0)
        inputs[2].wait()

    if do_rows:
        first_axis = jnp.where(core == 0, x, y)
        last_axis = jnp.where(core == 0, y, x)
        turn_cap, last_cap = mid_ref.shape[1], rows_ref.shape[1]

        def pack(half, line):
            row = jnp.zeros((turn_cap, 1), F32)
            for i in range(side):
                dest = line_device(half, line, i)
                key, val = key_ref[pl.ds(dest, 1), :], local_ref[pl.ds(dest, 1), :]
                row += jnp.sum(jnp.where(key == iota((turn_cap, tokens), 0), val, 0.0), axis=1, keepdims=True)
            hot_ref[...] = (row - 1.0 == iota((turn_cap, vocab), 1)).astype(BF16)
            return jnp.dot(hot_ref[...], table_ref[...], preferred_element_type=F32).astype(BF16)

        inputs[4].wait()
        bundles = []
        for step in (2, 1, 3):
            for half in range(2):
                at, here = len(bundles), (x, y)[half]
                pack_ref[at] = pack(half, lax.rem(here + step, side))
                target = ((y * side + lax.rem(x + step, side)) * 2, (lax.rem(y + step, side) * side + x) * 2 + 1)[half]
                bundles.append((pack_ref.at[at], mid_ref.at[here * 2 + core], mid_sem.at[step * 2 + core], target))
                if at == 0:
                    enter()
                else:
                    send(*bundles[-2])
        pack_ref[len(bundles)] = pack(1 - core, last_axis)
        send(*bundles[-1])
        own()
        mid_ref[first_axis * 2 + core] = pack(core, first_axis)
        send(pack_ref.at[len(bundles)], mid_ref.at[last_axis * 2 + core], mid_sem.at[0], device(0, 0, 1))

        j = lax.broadcasted_iota(jnp.int32, (2 * side, 1), 0)
        source = jnp.where(core == 0, y * (2 * side) + j, (j >> 1) * (2 * side) + x * 2 + (j & 1)).astype(F32)
        for i in range(side):
            mine = owner_ref[pl.ds(line_device(core, first_axis, i), 1), :]
            turn_ref[i * 2 * side:(i + 1) * 2 * side, :] = ones(mine == source)
        from_source = turn_ref[...]
        in_block = count_before(from_source)
        r, c = iota((n, n), 0), iota((n, n), 1)
        (ri, _, _), (ci, _, _) = coords(r, side), coords(c, side)
        earlier = (r - ri * (2 * side) == c - ci * (2 * side)) & (ci < ri)
        in_line = jnp.dot(ones(earlier).astype(BF16), from_source.astype(BF16), preferred_element_type=F32)
        slot = in_block + jnp.sum(in_line, axis=1, keepdims=True) + 1.0
        for i in range(side):
            part = slice(i * 2 * side, (i + 1) * 2 * side)
            mask = from_source[part]
            at = jnp.sum(mask * (slot[part] + j.astype(F32) * turn_cap), axis=0, keepdims=True)
            rank = jnp.sum(in_block[part], axis=0, keepdims=True)
            key_ref[i:i + 1, :] = jnp.where(at > 0, rank, -1.0)
            local_ref[i:i + 1, :] = at

        own_y, own_x, _ = coords(owner_ref[pl.ds(me, 1), :], side)
        via, place = place_among(jnp.where(core == 0, own_y, own_x))
        slot = via * last_cap + place

        def count(owner, counts):
            here = jnp.sum(ones(owner_ref[...] == owner.astype(F32)), axis=1, keepdims=True)
            return jnp.where(iota(counts.shape, 1) == owner.astype(F32), here, counts)

        counts = lax.fori_loop(0, n, count, jnp.zeros((n, 128), F32))
        exact = functools.partial(jnp.dot, precision=lax.Precision.HIGHEST, preferred_element_type=F32)
        in_bundle = exact(same_line, counts)
        oy, ox, _ = coords(iota((128, 128), 0), side)
        g = iota((128, 128), 1)
        blocks = exact(counts, ones((oy == g) | ((oy < side) & (ox == g - side))))
        lane = iota((n, 128), 1)
        dest_core = coords(iota((n, 128), 0), side)[2]
        counted = jnp.where(dest_core == 0, ones(lane < side), ones((lane >= side) & (lane < 2 * side)))
        over = ones(in_bundle > turn_cap) + counted * ones(blocks > last_cap)
        over_ref[0] = jnp.max(over)
        worst_ref[0] = jnp.max(counts)

        got_all("10 30")
        spread(1)
        wait(mid_ref.at[first_axis * 2 + 1 - core], mid_sem.at[0])
        for step in (1, 3, 2):
            for sc in range(2):
                wait(mid_ref.at[lax.rem(first_axis - step + side, side) * 2 + sc], mid_sem.at[step * 2 + sc])

        def turn(step):
            i = lax.rem(last_axis + step, side)
            key, val = key_ref[pl.ds(i, 1), :], local_ref[pl.ds(i, 1), :]
            row = jnp.sum(jnp.where(key == iota((last_cap, tokens), 0), val, 0.0), axis=1, keepdims=True) - 1.0
            hot = (row == iota((last_cap, 2 * side * turn_cap), 1)).astype(BF16)
            return jnp.dot(hot, mid_ref[...].reshape(2 * side * turn_cap, -1), preferred_element_type=F32).astype(BF16)

        def send_turn(step):
            send(last_ref.at[step], rows_ref.at[last_axis], rows_sem.at[step],
                 jnp.where(core == 0, device(step, 0), device(0, step)))

        last_ref[2] = turn(2)
        last_ref[1] = turn(1)
        send_turn(2)
        last_ref[3] = turn(3)
        send_turn(1)
        rows_ref[last_axis] = turn(0)
        send_turn(3)
        got_all("01 03 20")
        spread(2)
        got_all("11 13")
        spread(3)

        for step in (1, 3, 2):
            wait(rows_ref.at[lax.rem(last_axis - step + side, side)], rows_sem.at[step])
        hot = (slot == iota((tokens, side * last_cap), 1)).astype(BF16)
        x_ref[...] = jnp.dot(hot, rows_ref[...].reshape(side * last_cap, -1), preferred_element_type=F32).astype(BF16)
    else:
        x_ref[...] = x_in_ref[...]
        enter()
        own()
        got_all("10 30")
        spread(1, 3)
        got_all("20")
        spread(2)
        for spots in ("01 03 11 13", "31 33 21 23", "02 12 32 22"):
            got_all(spots)

    gain = jnp.concatenate([gain_ref[i:i + 1, :] for i in range(gain_ref.shape[0])], axis=1).astype(F32)
    rows = x_ref[...].astype(F32)
    inv_rms = lax.rsqrt(jnp.mean(rows * rows, axis=-1, keepdims=True) + RMS_EPS)
    n_ref[...] = (rows * inv_rms * gain).astype(BF16)
    acc_ref[...] = jnp.zeros_like(acc_ref)
    span = 2 * w_all.shape[5]

    def mlp(spots, owner_core=None):
        spots = parse(spots) if isinstance(spots, str) else spots
        cores = slice(None) if owner_core is None else pl.ds(owner_core, 1)
        rows = span if owner_core is None else span // 2
        width = 2 * len(spots) * rows
        for part, dst in enumerate((w1_ref, w2_ref)):
            at = 0
            for a, b in spots:
                for dx, dy, half in ((a, b, 0), (b, a, 1)):
                    row, col = lax.rem(y - dy + side, side), lax.rem(x - dx + side, side)
                    dst[at:at + rows] = w_all[row, col, cores, half, part].reshape(rows, -1)
                    at += rows

        u = lax.dot_general(n_ref[...], w1_ref[:width], (((1,), (1,)), ((), ())), preferred_element_type=F32)
        h = gelu(u.astype(BF16).astype(F32)).astype(BF16)
        acc_ref[...] += jnp.dot(h, w2_ref[:width], preferred_element_type=F32)

    if do_rows:
        from_sibling("00 10 20 30")
        mlp("00 10 20 30")
        got_all("02 21 23")
        from_sibling("01 03 11 13")
        mlp("01 03 11 13")
        got_all("12")
        mlp("02 12 21 23", core)
        from_sibling("02 21 23 12")
        mlp("02 12 21 23", 1 - core)
        got_all("31 33 32 22")
        mlp("31 33 32 22", core)
        from_sibling("31 33 32 22")
        mlp("31 33 32 22", 1 - core)
    else:
        def every(a, carry):
            mlp([(a, b) for b in range(side)])
            return carry

        for spots in ("00 01 02 03", "10 11 12 13", "20 21 22 23", "30 31 32 33"):
            from_sibling(spots)
        lax.fori_loop(0, side, every, 0)
    out_ref[...] = (x_ref[...].astype(F32) + acc_ref[...]).astype(BF16)
    for copy in sent:
        copy.wait_send()


def params(collective_id):
    return pltpu.CompilerParams(collective_id=collective_id, has_side_effects=True, vmem_limit_bytes=VMEM_LIMIT)


def rows_call(n, tokens, dim, vocab):
    vmem, dma = pltpu.VMEM, pltpu.SemaphoreType.DMA
    spec = pl.BlockSpec(memory_space=pltpu.VMEM)
    return pl.pallas_call(
        functools.partial(rows_kernel, n, CAP),
        out_shape=jax.ShapeDtypeStruct((tokens, dim), BF16),
        in_specs=[pl.BlockSpec(memory_space=pltpu.SMEM), spec, spec],
        out_specs=spec,
        scratch_shapes=[vmem((n, tokens), F32), vmem((n, tokens), F32), vmem((GROUP, CAP, vocab), BF16),
                        vmem((n, CAP, dim), BF16), vmem((n, CAP, dim), BF16), vmem((tokens, dim), F32),
                        dma((n,)), dma((n,))],
        compiler_params=params(0))


def block_call(n, side, do_rows, tokens, dim, vocab, share):
    vmem, dma = pltpu.VMEM, pltpu.SemaphoreType.DMA
    spec, hbm = pl.BlockSpec(memory_space=pltpu.VMEM), pl.BlockSpec(memory_space=pltpu.HBM)
    out_shape = [jax.ShapeDtypeStruct((tokens, dim), BF16)]
    sends = 2 * (4 + 16 - len(DIRECT) + side * side) + (7 + 3 if do_rows else 0)
    scratch = [vmem((dim // 128, 128), BF16), vmem((tokens, dim), BF16), vmem((tokens, dim), F32),
               vmem((side, side, 2, 2, 2, share // 2, dim), BF16), vmem((n * share // side, dim), BF16),
               vmem((n * share // side, dim), BF16), vmem((tokens, dim), BF16),
               dma((sends,)), dma((2, 2, side * side)), dma((2, side * side)), dma((5,))]
    if do_rows:
        out_shape += [jax.ShapeDtypeStruct((1,), F32)] * 2
        scratch += [vmem((n * tokens // 128, 128), jnp.int32), vmem((vocab, dim), BF16)] + [vmem((n, tokens), F32)] * 3 + [
            vmem((TURN_CAP, vocab), BF16), vmem((2 * side - 1, TURN_CAP, dim), BF16), vmem((2 * side, TURN_CAP, dim), BF16),
            vmem((n, tokens), F32), vmem((side, LAST_CAP, dim), BF16), vmem((side, LAST_CAP, dim), BF16),
            dma((2 * side,)), dma((side,))]
    return pl.pallas_call(
        functools.partial(block_kernel, n, side, do_rows),
        out_shape=out_shape,
        in_specs=([hbm, hbm] if do_rows else [spec]) + [hbm] * 3,
        out_specs=[spec] + [pl.BlockSpec(memory_space=pltpu.SMEM)] * (len(out_shape) - 1),
        scratch_shapes=scratch,
        compiler_params=params(1 + do_rows))


def solution(mesh):
    n = mesh.shape["tp"]
    side = math.isqrt(n // 2)

    def device_step(token_ids, table_shard, norm_gain, w_in_shard, w_out_shard):
        vocab, dim = table_shard.shape
        share = w_out_shard.shape[0]
        tokens = token_ids.shape[0] // n
        ids = token_ids.reshape(n, tokens)
        block = (norm_gain.reshape(dim // 128, 128), w_in_shard.T.reshape(2, share // 2, dim),
                 w_out_shard.reshape(2, share // 2, dim))
        out, over, worst = block_call(n, side, True, tokens, dim, vocab, share)(
            token_ids.reshape(n * tokens // 128, 128), table_shard, *block)

        def in_rounds():
            rounds = lax.div(worst[0].astype(jnp.int32) + CAP - 1, CAP)

            def one(carry):
                r, rows = carry
                return r + 1, rows + rows_call(n, tokens, dim, vocab)(r.reshape(1), ids, table_shard)

            _, rows = lax.while_loop(lambda carry: carry[0] < rounds, one,
                                     (jnp.int32(0), jnp.zeros((tokens, dim), BF16)))
            return block_call(n, side, False, tokens, dim, vocab, share)(rows, *block)[0]

        return lax.cond(over[0] > 0, in_rounds, lambda: out)

    return jax.shard_map(
        device_step,
        mesh=mesh,
        in_specs=(P("dp"), P("tp", None), P(), P(None, "tp"), P("tp", None)),
        out_specs=P(("dp", "tp"), None),
        check_vma=False,
    )
```

```python
import functools
import math

import jax
import jax.numpy as jnp
from jax import lax
from jax.experimental import pallas as pl
from jax.experimental.pallas import tpu as pltpu
from jax.sharding import PartitionSpec as P

RMS_EPS = 1e-6
MESH = pl.DeviceIdType.MESH
TURN_CAP, LAST_CAP = 224, 272
CAP, GROUP = 64, 8
VMEM_LIMIT = 44 * 2**20
DIRECT = (3,)
GELU_SCALE = math.sqrt(2.0 / math.pi)
F32, BF16 = jnp.float32, jnp.bfloat16


def iota(shape, dim):
    return lax.broadcasted_iota(jnp.int32, shape, dim).astype(F32)


def ones(mask):
    return jnp.where(mask, 1.0, 0.0)


def count_before(mask):
    tokens = mask.shape[1]
    before = ones(iota((tokens, tokens), 0) < iota((tokens, tokens), 1)).astype(BF16)
    return jnp.dot(mask.astype(BF16), before, preferred_element_type=F32)


def as_column(row):
    tokens = row.shape[1]
    return jnp.sum(jnp.where(iota((tokens, tokens), 0) == iota((tokens, tokens), 1), row, 0.0), axis=1, keepdims=True)


def place_among(kind):
    column = as_column(kind)
    tokens = kind.shape[1]
    same = (column == kind) & (iota((tokens, tokens), 1) < iota((tokens, tokens), 0))
    return column, jnp.sum(ones(same), axis=1, keepdims=True)


def coords(device, side):
    y = jnp.floor((device + 0.5) * (0.5 / side))
    x = jnp.floor((device - y * (2 * side) + 0.5) * 0.5)
    return y, x, device - y * (2 * side) - x * 2


def owner_of(ids, vocab):
    return jnp.floor((ids + 0.5) * (1.0 / vocab))


def gelu(z):
    return (0.5 * z) * (1.0 + jnp.tanh(z * (GELU_SCALE + GELU_SCALE * 0.044715 * (z * z))))


def by_destination(ids_ref, n):
    each = ids_ref.shape[0] // n
    return jnp.concatenate([ids_ref[pl.ds(j, n, stride=each), :] for j in range(each)], axis=1).astype(F32)


def greet_all(n, me):
    def greet(k, carry):
        pl.semaphore_signal(pltpu.get_barrier_semaphore(), inc=1, device_id={"tp": lax.rem(me + k, n)},
                            device_id_type=MESH)
        return carry

    lax.fori_loop(1, n, greet, 0)


def remote(src, dst, send_sem, recv_sem, target):
    return pltpu.make_async_remote_copy(src_ref=src, dst_ref=dst, send_sem=send_sem, recv_sem=recv_sem,
                                        device_id={"tp": target}, device_id_type=MESH)


def rows_kernel(n, cap, round_ref, ids_ref, table_ref, out_ref, key_ref, local_ref, hot_ref, pack_ref, rows_ref, acc_ref,
                send_sem, rows_sem):
    vocab, tokens = table_ref.shape[0], ids_ref.shape[1]
    me = lax.axis_index("tp")
    greet_all(n, me)
    local = ids_ref[...].astype(F32) - (me * vocab).astype(F32)
    owned = (local >= 0) & (local < vocab)
    first = (round_ref[0] * cap).astype(F32)
    key_ref[...] = jnp.where(owned, count_before(ones(owned)) - first, -1.0)
    local_ref[...] = local + 1.0
    pl.semaphore_wait(pltpu.get_barrier_semaphore(), n - 1)

    def pack(group, carry):
        def fill(j, carry):
            dest = lax.rem(me + group * GROUP + j, n)
            key, val = key_ref[pl.ds(dest, 1), :], local_ref[pl.ds(dest, 1), :]
            row = jnp.sum(jnp.where(key == iota((cap, tokens), 0), val, 0.0), axis=1, keepdims=True) - 1.0
            hot_ref[j] = (row == iota((cap, vocab), 1)).astype(BF16)
            return carry

        lax.fori_loop(0, GROUP, fill, 0)
        rows = jnp.dot(hot_ref[...].reshape(GROUP * cap, vocab), table_ref[...], preferred_element_type=F32)
        pack_ref[pl.ds(group * GROUP, GROUP)] = rows.astype(BF16).reshape(GROUP, cap, -1)
        return carry

    lax.fori_loop(0, n // GROUP, pack, 0)

    def pair(k, source):
        return remote(pack_ref.at[k], rows_ref.at[source], send_sem.at[k], rows_sem.at[k], lax.rem(me + k, n))

    def start(k, carry):
        pair(k, me).start()
        return carry

    lax.fori_loop(1, n, start, 0)
    rows_ref[me] = pack_ref[0]
    owner, place = place_among(owner_of(ids_ref[pl.ds(me, 1), :].astype(F32), vocab))
    place = place - first
    slot = jnp.where((place >= 0) & (place < cap), owner * cap + place, -1.0)

    def finish(k, carry):
        pair(k, lax.rem(me - k + n, n)).wait_recv()
        pair(k, me).wait_send()
        return carry

    lax.fori_loop(1, n, finish, 0)
    acc_ref[...] = jnp.zeros_like(acc_ref)

    def unpack(group, carry):
        hot = (slot - (group * (GROUP * cap)).astype(F32) == iota((tokens, GROUP * cap), 1)).astype(BF16)
        acc_ref[...] += jnp.dot(hot, rows_ref[pl.ds(group * GROUP, GROUP)].reshape(GROUP * cap, -1),
                                preferred_element_type=F32)
        return carry

    lax.fori_loop(0, n // GROUP, unpack, 0)
    out_ref[...] = acc_ref[...].astype(BF16)


def block_kernel(n, side, do_rows, *refs):
    refs = list(refs)
    take = lambda count: [refs.pop(0) for _ in range(count)]
    if do_rows:
        ids_in, table_in = take(2)
    else:
        (x_in_ref,) = take(1)
    gain_in, w1_in, w2_in, out_ref = take(4)
    if do_rows:
        over_ref, worst_ref = take(2)
    gain_ref, x_ref, acc_ref, w_all, w1_ref, w2_ref, n_ref, send_sem, w_sem, sib_sem, in_sem = take(11)
    if do_rows:
        (ids_ref, table_ref, key_ref, local_ref, owner_ref, hot_ref, pack_ref, mid_ref, turn_ref, last_ref, rows_ref,
         mid_sem, rows_sem) = take(13)
        vocab, tokens = table_ref.shape[0], key_ref.shape[1]

    me = lax.axis_index("tp")
    y, x, core = me // (2 * side), (me // 2) % side, me % 2

    def device(dy, dx, dc=0):
        return (lax.rem(y + dy + side, side) * side + lax.rem(x + dx + side, side)) * 2 + lax.rem(core + dc, 2)

    sent = []

    def send(src, dst, recv_sem, target):
        copy = remote(src, dst, send_sem.at[len(sent)], recv_sem, target)
        copy.start()
        sent.append(copy)

    def wait(ref, recv_sem):
        remote(ref, ref, send_sem.at[0], recv_sem, me).wait_recv()

    partners = [device(0, 0, 1)]
    for step in (2, 1, 3):
        for other in range(2):
            partners += [device(0, step, other), device(step, 0, other)]
    for partner in partners:
        pl.semaphore_signal(pltpu.get_barrier_semaphore(), inc=1, device_id={"tp": partner}, device_id_type=MESH)
    inputs = [pltpu.make_async_copy(part_in, w_all.at[y, x, core, :, part], in_sem.at[part])
              for part, part_in in enumerate((w1_in, w2_in))]
    inputs += [pltpu.make_async_copy(gain_in, gain_ref, in_sem.at[2])]
    if do_rows:
        inputs += [pltpu.make_async_copy(ids_in, ids_ref, in_sem.at[3]),
                   pltpu.make_async_copy(table_in, table_ref, in_sem.at[4])]
        inputs[3].start()
    for copy in inputs[:3] + inputs[4:]:
        copy.start()

    def piece(half, a, b, owner_core):
        dx, dy = (a, b) if half == 0 else (b, a)
        return w_all.at[lax.rem(y - dy + side, side), lax.rem(x - dx + side, side), owner_core, half]

    def along(half, first, step):
        return device(0, step) if (half == 0) == first else device(step, 0)

    def spot(a, b):
        return a * side + b

    def second_axis(half, a):
        here = piece(half, a, 0, core)
        if a in DIRECT:
            send(here, here, w_sem.at[half, 0, spot(a, 2)], along(half, False, 2))
        send(here, here, w_sem.at[half, 0, spot(a, 1)], along(half, False, 1))
        send(here, here, w_sem.at[half, 0, spot(a, 3)], along(half, False, -1))

    def to_sibling(half, a, b):
        here = piece(half, a, b, core)
        send(here, here, sib_sem.at[half, spot(a, b)], device(0, 0, 1))

    def got(half, a, b):
        here = piece(half, a, b, core)
        if (b == 2 and a not in DIRECT) or (a, b) == (2, 0):
            for part in range(2):
                wait(here.at[part], w_sem.at[half, part, spot(a, b)])
        else:
            wait(here, w_sem.at[half, 0, spot(a, b)])
        if (a, b) == (1, 0):
            send(here.at[0], here.at[0], w_sem.at[half, 0, spot(2, 0)], along(half, True, 1))
        if (a, b) == (3, 0):
            send(here.at[1], here.at[1], w_sem.at[half, 1, spot(2, 0)], along(half, True, -1))
        if b == 1 and a not in DIRECT:
            send(here.at[0], here.at[0], w_sem.at[half, 0, spot(a, 2)], along(half, False, 1))
        if b == 3 and a not in DIRECT:
            send(here.at[1], here.at[1], w_sem.at[half, 1, spot(a, 2)], along(half, False, -1))
        to_sibling(half, a, b)

    def parse(spots):
        return [(int(a), int(b)) for a, b in spots.split()]

    def got_all(spots):
        for a, b in parse(spots):
            for half in range(2):
                got(half, a, b)

    def from_sibling(spots):
        for a, b in parse(spots):
            for half in range(2):
                wait(piece(half, a, b, 1 - core), sib_sem.at[half, spot(a, b)])

    def spread(*firsts):
        for a in firsts:
            for half in range(2):
                second_axis(half, a)

    def line_device(half, line, i):
        in_x, in_y = (i * side + line) * 2, (line * side + i) * 2 + 1
        return in_x if isinstance(half, int) and half == 0 else in_y if isinstance(half, int) else jnp.where(half == 0, in_x, in_y)

    if do_rows:
        inputs[3].wait()
        ids = by_destination(ids_ref, n)
        local = ids - (me * vocab).astype(F32)
        owned = ones((local >= 0) & (local < vocab))
        dy, dx, dc = coords(iota((n, n), 0), side)
        ey, ex, ec = coords(iota((n, n), 1), side)
        same_line = ones(dc == ec) * jnp.where(dc == 0, ones(dx == ex), ones(dy == ey))
        earlier = same_line * jnp.where(dc == 0, ones(ey < dy), ones(ex < dx))
        in_line = jnp.dot(earlier.astype(BF16), owned.astype(BF16), preferred_element_type=F32)
        rank = count_before(owned) + jnp.sum(in_line, axis=1, keepdims=True)
        key_ref[...] = jnp.where(owned > 0, rank, -1.0)
        local_ref[...] = local + 1.0
        owner_ref[...] = owner_of(ids, vocab)

    def enter():
        inputs[0].wait()
        inputs[1].wait()
        pl.semaphore_wait(pltpu.get_barrier_semaphore(), len(partners))
        for half in range(2):
            here = piece(half, 0, 0, core)
            send(here, here, w_sem.at[half, 0, spot(1, 0)], along(half, True, 1))
            send(here, here, w_sem.at[half, 0, spot(3, 0)], along(half, True, -1))

    def own():
        spread(0)
        for half in range(2):
            to_sibling(half, 0, 0)
        inputs[2].wait()

    if do_rows:
        first_axis = jnp.where(core == 0, x, y)
        last_axis = jnp.where(core == 0, y, x)
        turn_cap, last_cap = mid_ref.shape[1], rows_ref.shape[1]

        def pack(half, line):
            row = jnp.zeros((turn_cap, 1), F32)
            for i in range(side):
                dest = line_device(half, line, i)
                key, val = key_ref[pl.ds(dest, 1), :], local_ref[pl.ds(dest, 1), :]
                row += jnp.sum(jnp.where(key == iota((turn_cap, tokens), 0), val, 0.0), axis=1, keepdims=True)
            hot_ref[...] = (row - 1.0 == iota((turn_cap, vocab), 1)).astype(BF16)
            return jnp.dot(hot_ref[...], table_ref[...], preferred_element_type=F32).astype(BF16)

        inputs[4].wait()
        bundles = []
        for step in (2, 1, 3):
            for half in range(2):
                at, here = len(bundles), (x, y)[half]
                pack_ref[at] = pack(half, lax.rem(here + step, side))
                target = ((y * side + lax.rem(x + step, side)) * 2, (lax.rem(y + step, side) * side + x) * 2 + 1)[half]
                bundles.append((pack_ref.at[at], mid_ref.at[here * 2 + core], mid_sem.at[step * 2 + core], target))
                if at == 0:
                    enter()
                else:
                    send(*bundles[-2])
        pack_ref[len(bundles)] = pack(1 - core, last_axis)
        send(*bundles[-1])
        own()
        mid_ref[first_axis * 2 + core] = pack(core, first_axis)
        send(pack_ref.at[len(bundles)], mid_ref.at[last_axis * 2 + core], mid_sem.at[0], device(0, 0, 1))

        j = lax.broadcasted_iota(jnp.int32, (2 * side, 1), 0)
        source = jnp.where(core == 0, y * (2 * side) + j, (j >> 1) * (2 * side) + x * 2 + (j & 1)).astype(F32)
        for i in range(side):
            mine = owner_ref[pl.ds(line_device(core, first_axis, i), 1), :]
            turn_ref[i * 2 * side:(i + 1) * 2 * side, :] = ones(mine == source)
        from_source = turn_ref[...]
        in_block = count_before(from_source)
        r, c = iota((n, n), 0), iota((n, n), 1)
        (ri, _, _), (ci, _, _) = coords(r, side), coords(c, side)
        earlier = (r - ri * (2 * side) == c - ci * (2 * side)) & (ci < ri)
        in_line = jnp.dot(ones(earlier).astype(BF16), from_source.astype(BF16), preferred_element_type=F32)
        slot = in_block + jnp.sum(in_line, axis=1, keepdims=True) + 1.0
        for i in range(side):
            part = slice(i * 2 * side, (i + 1) * 2 * side)
            mask = from_source[part]
            at = jnp.sum(mask * (slot[part] + j.astype(F32) * turn_cap), axis=0, keepdims=True)
            rank = jnp.sum(in_block[part], axis=0, keepdims=True)
            key_ref[i:i + 1, :] = jnp.where(at > 0, rank, -1.0)
            local_ref[i:i + 1, :] = at

        own_y, own_x, _ = coords(owner_ref[pl.ds(me, 1), :], side)
        via, place = place_among(jnp.where(core == 0, own_y, own_x))
        slot = via * last_cap + place

        def count(owner, counts):
            here = jnp.sum(ones(owner_ref[...] == owner.astype(F32)), axis=1, keepdims=True)
            return jnp.where(iota(counts.shape, 1) == owner.astype(F32), here, counts)

        counts = lax.fori_loop(0, n, count, jnp.zeros((n, 128), F32))
        exact = functools.partial(jnp.dot, precision=lax.Precision.HIGHEST, preferred_element_type=F32)
        in_bundle = exact(same_line, counts)
        oy, ox, _ = coords(iota((128, 128), 0), side)
        g = iota((128, 128), 1)
        blocks = exact(counts, ones((oy == g) | ((oy < side) & (ox == g - side))))
        lane = iota((n, 128), 1)
        dest_core = coords(iota((n, 128), 0), side)[2]
        counted = jnp.where(dest_core == 0, ones(lane < side), ones((lane >= side) & (lane < 2 * side)))
        over = ones(in_bundle > turn_cap) + counted * ones(blocks > last_cap)
        over_ref[0] = jnp.max(over)
        worst_ref[0] = jnp.max(counts)

        got_all("10 30")
        spread(1)
        wait(mid_ref.at[first_axis * 2 + 1 - core], mid_sem.at[0])
        for step in (1, 3, 2):
            for sc in range(2):
                wait(mid_ref.at[lax.rem(first_axis - step + side, side) * 2 + sc], mid_sem.at[step * 2 + sc])

        def turn(step):
            i = lax.rem(last_axis + step, side)
            key, val = key_ref[pl.ds(i, 1), :], local_ref[pl.ds(i, 1), :]
            row = jnp.sum(jnp.where(key == iota((last_cap, tokens), 0), val, 0.0), axis=1, keepdims=True) - 1.0
            hot = (row == iota((last_cap, 2 * side * turn_cap), 1)).astype(BF16)
            return jnp.dot(hot, mid_ref[...].reshape(2 * side * turn_cap, -1), preferred_element_type=F32).astype(BF16)

        def send_turn(step):
            send(last_ref.at[step], rows_ref.at[last_axis], rows_sem.at[step],
                 jnp.where(core == 0, device(step, 0), device(0, step)))

        last_ref[2] = turn(2)
        last_ref[1] = turn(1)
        send_turn(2)
        last_ref[3] = turn(3)
        send_turn(1)
        rows_ref[last_axis] = turn(0)
        send_turn(3)
        got_all("01 03 20")
        spread(2)
        got_all("11 13")
        spread(3)

        for step in (1, 3, 2):
            wait(rows_ref.at[lax.rem(last_axis - step + side, side)], rows_sem.at[step])
        hot = (slot == iota((tokens, side * last_cap), 1)).astype(BF16)
        x_ref[...] = jnp.dot(hot, rows_ref[...].reshape(side * last_cap, -1), preferred_element_type=F32).astype(BF16)
    else:
        x_ref[...] = x_in_ref[...]
        enter()
        own()
        got_all("10 30")
        spread(1, 3)
        got_all("20")
        spread(2)
        for spots in ("01 03 11 13", "31 33 21 23", "02 12 32 22"):
            got_all(spots)

    gain = jnp.concatenate([gain_ref[i:i + 1, :] for i in range(gain_ref.shape[0])], axis=1).astype(F32)
    rows = x_ref[...].astype(F32)
    inv_rms = lax.rsqrt(jnp.mean(rows * rows, axis=-1, keepdims=True) + RMS_EPS)
    n_ref[...] = (rows * inv_rms * gain).astype(BF16)
    if not do_rows:
        acc_ref[...] = jnp.zeros_like(acc_ref)
    span = 2 * w_all.shape[5]

    def mlp(spots, owner_core=None, first=False):
        spots = parse(spots) if isinstance(spots, str) else spots
        cores = slice(None) if owner_core is None else pl.ds(owner_core, 1)
        rows = span if owner_core is None else span // 2
        width = 2 * len(spots) * rows
        for part, dst in enumerate((w1_ref, w2_ref)):
            at = 0
            for a, b in spots:
                for dx, dy, half in ((a, b, 0), (b, a, 1)):
                    row, col = lax.rem(y - dy + side, side), lax.rem(x - dx + side, side)
                    dst[at:at + rows] = w_all[row, col, cores, half, part].reshape(rows, -1)
                    at += rows

        u = lax.dot_general(n_ref[...], w1_ref[:width], (((1,), (1,)), ((), ())), preferred_element_type=F32)
        h = gelu(u.astype(BF16).astype(F32)).astype(BF16)
        part = jnp.dot(h, w2_ref[:width], preferred_element_type=F32)
        acc_ref[...] = part if first else acc_ref[...] + part

    if do_rows:
        from_sibling("00 10 20 30")
        mlp("00 10 20 30", first=True)
        got_all("02 21 23")
        from_sibling("01 03 11 13")
        mlp("01 03 11 13")
        got_all("12")
        mlp("02 12 21 23", core)
        from_sibling("02 21 23 12")
        mlp("02 12 21 23", 1 - core)
        got_all("31 33 32 22")
        mlp("31 33 32 22", core)
        from_sibling("31 33 32 22")
        mlp("31 33 32 22", 1 - core)
    else:
        def every(a, carry):
            mlp([(a, b) for b in range(side)])
            return carry

        for spots in ("00 01 02 03", "10 11 12 13", "20 21 22 23", "30 31 32 33"):
            from_sibling(spots)
        lax.fori_loop(0, side, every, 0)
    out_ref[...] = (x_ref[...].astype(F32) + acc_ref[...]).astype(BF16)
    for copy in sent:
        copy.wait_send()


def params(collective_id):
    return pltpu.CompilerParams(collective_id=collective_id, has_side_effects=True, vmem_limit_bytes=VMEM_LIMIT)


def rows_call(n, tokens, dim, vocab):
    vmem, dma = pltpu.VMEM, pltpu.SemaphoreType.DMA
    spec = pl.BlockSpec(memory_space=pltpu.VMEM)
    return pl.pallas_call(
        functools.partial(rows_kernel, n, CAP),
        out_shape=jax.ShapeDtypeStruct((tokens, dim), BF16),
        in_specs=[pl.BlockSpec(memory_space=pltpu.SMEM), spec, spec],
        out_specs=spec,
        scratch_shapes=[vmem((n, tokens), F32), vmem((n, tokens), F32), vmem((GROUP, CAP, vocab), BF16),
                        vmem((n, CAP, dim), BF16), vmem((n, CAP, dim), BF16), vmem((tokens, dim), F32),
                        dma((n,)), dma((n,))],
        compiler_params=params(0))


def block_call(n, side, do_rows, tokens, dim, vocab, share):
    vmem, dma = pltpu.VMEM, pltpu.SemaphoreType.DMA
    spec, hbm = pl.BlockSpec(memory_space=pltpu.VMEM), pl.BlockSpec(memory_space=pltpu.HBM)
    out_shape = [jax.ShapeDtypeStruct((tokens, dim), BF16)]
    sends = 2 * (4 + 16 - len(DIRECT) + side * side) + (7 + 3 if do_rows else 0)
    scratch = [vmem((dim // 128, 128), BF16), vmem((tokens, dim), BF16), vmem((tokens, dim), F32),
               vmem((side, side, 2, 2, 2, share // 2, dim), BF16), vmem((n * share // side, dim), BF16),
               vmem((n * share // side, dim), BF16), vmem((tokens, dim), BF16),
               dma((sends,)), dma((2, 2, side * side)), dma((2, side * side)), dma((5,))]
    if do_rows:
        out_shape += [jax.ShapeDtypeStruct((1,), F32)] * 2
        scratch += [vmem((n * tokens // 128, 128), jnp.int32), vmem((vocab, dim), BF16)] + [vmem((n, tokens), F32)] * 3 + [
            vmem((TURN_CAP, vocab), BF16), vmem((2 * side - 1, TURN_CAP, dim), BF16), vmem((2 * side, TURN_CAP, dim), BF16),
            vmem((n, tokens), F32), vmem((side, LAST_CAP, dim), BF16), vmem((side, LAST_CAP, dim), BF16),
            dma((2 * side,)), dma((side,))]
    return pl.pallas_call(
        functools.partial(block_kernel, n, side, do_rows),
        out_shape=out_shape,
        in_specs=([hbm, hbm] if do_rows else [spec]) + [hbm] * 3,
        out_specs=[spec] + [pl.BlockSpec(memory_space=pltpu.SMEM)] * (len(out_shape) - 1),
        scratch_shapes=scratch,
        compiler_params=params(1 + do_rows))


def solution(mesh):
    n = mesh.shape["tp"]
    side = math.isqrt(n // 2)

    def device_step(token_ids, table_shard, norm_gain, w_in_shard, w_out_shard):
        vocab, dim = table_shard.shape
        share = w_out_shard.shape[0]
        tokens = token_ids.shape[0] // n
        ids = token_ids.reshape(n, tokens)
        block = (norm_gain.reshape(dim // 128, 128), w_in_shard.T.reshape(2, share // 2, dim),
                 w_out_shard.reshape(2, share // 2, dim))
        out, over, worst = block_call(n, side, True, tokens, dim, vocab, share)(
            token_ids.reshape(n * tokens // 128, 128), table_shard, *block)

        def in_rounds():
            rounds = lax.div(worst[0].astype(jnp.int32) + CAP - 1, CAP)

            def one(carry):
                r, rows = carry
                return r + 1, rows + rows_call(n, tokens, dim, vocab)(r.reshape(1), ids, table_shard)

            _, rows = lax.while_loop(lambda carry: carry[0] < rounds, one,
                                     (jnp.int32(0), jnp.zeros((tokens, dim), BF16)))
            return block_call(n, side, False, tokens, dim, vocab, share)(rows, *block)[0]

        return lax.cond(over[0] > 0, in_rounds, lambda: out)

    return jax.shard_map(
        device_step,
        mesh=mesh,
        in_specs=(P("dp"), P("tp", None), P(), P(None, "tp"), P("tp", None)),
        out_specs=P(("dp", "tp"), None),
        check_vma=False,
    )
```
